16 devices in a mesh: fsdp: 2 (over z), tp: 8 (over y, x, core).
Axes of the slice: x: 2, y: 2, z: 2, core: 2. Of those that a mesh axis runs over, the one named last changes fastest.
Arguments:
- x: bfloat16 [16384, 4096], P(('fsdp', 'tp'))
- gamma: float32 [4096], replicated
- w1: bfloat16 [4096, 16384], P('fsdp', 'tp')
- w2: bfloat16 [16384, 4096], P('tp', 'fsdp')
Outputs:
- output: bfloat16 [16384, 4096], P(('fsdp', 'tp'))
All inputs are finite; a program needn't handle non-finite values.
Results may differ from the reference program's by a relative error of at most 0.001.
Values are sent between devices in bfloat16 or wider.
A program may use at most 1 GiB of HBM per device.

```python
import jax
import jax.numpy as jnp
from jax import lax

D = 4096
F = 16384
ROWS = 1024
FSDP = 2
TP = 8

TOK = FSDP * TP * ROWS
BLK = min(ROWS, 512)
EPS = 1e-6


def setup_inputs(seed: int = 0) -> dict:
    k = jax.random.split(jax.random.key(seed), 4)
    x = jax.random.normal(k[0], (TOK, D), jnp.float32).astype(jnp.bfloat16)
    gamma = jax.random.uniform(k[1], (D,), jnp.float32, 0.5, 1.5)
    w1 = (jax.random.normal(k[2], (D, F), jnp.float32) * D ** -0.5).astype(jnp.bfloat16)
    w2 = (jax.random.normal(k[3], (F, D), jnp.float32) * F ** -0.5).astype(jnp.bfloat16)
    return {"x": x, "gamma": gamma, "w1": w1, "w2": w2}


def _block(x, gamma, w1, w2):
    xf = x.astype(jnp.float32)
    mu = jnp.mean(xf, axis=-1, keepdims=True)
    var = jnp.mean(jnp.square(xf - mu), axis=-1, keepdims=True)
    xn = ((xf - mu) * lax.rsqrt(var + EPS) * gamma).astype(jnp.bfloat16)
    h = jax.nn.gelu(jnp.dot(xn, w1, preferred_element_type=jnp.float32), approximate=True).astype(jnp.bfloat16)
    y = jnp.dot(h, w2, preferred_element_type=jnp.float32)
    return (xf + y).astype(jnp.bfloat16)


def reference(x, gamma, w1, w2):
    xb = x.reshape(TOK // BLK, BLK, D)
    yb = lax.map(lambda blk: _block(blk, gamma, w1, w2), xb)
    return yb.reshape(TOK, D)
```

```python
import jax
import jax.numpy as jnp
from jax import lax
from jax.sharding import PartitionSpec as P

EPS = 1e-6
AXES = ("fsdp", "tp")
CORE, X, Y, Z = 1, 2, 4, 8


def _norm(x, gamma):
    xf = x.astype(jnp.float32)
    mu = jnp.mean(xf, axis=-1, keepdims=True)
    var = jnp.mean(jnp.square(xf - mu), axis=-1, keepdims=True)
    return xf, ((xf - mu) * lax.rsqrt(var + EPS) * gamma).astype(jnp.bfloat16)


def _to(a, bit):
    return lax.ppermute(a, AXES, [(i, i ^ bit) for i in range(16)])


def _dot(a, b):
    return jnp.dot(a, b, preferred_element_type=jnp.float32)


def _gather(pieces):
    n = len(pieces)
    from_y, from_z, diag = [None] * n, [None] * n, [None] * n
    for c in range(n):
        from_y[c] = _to(pieces[c], Y)
        from_z[c] = _to(pieces[c], Z)
    for c in range(n):
        diag[c] = _to(from_z[c], Y) if c % 2 == 0 else _to(from_y[c], Z)
    both = lambda ps: [(p, _to(p, CORE)) for p in ps]
    return both(pieces), both(from_y), both(from_z), both(diag)


def solution(mesh):
    def body(x, gamma, w1, w2):
        z = lax.axis_index("fsdp")
        rows, d = x.shape
        half = d // 2
        n1, n2 = 4, 4
        c1, c2 = w1.shape[1] // n1, w2.shape[1] // n2

        xf, xn = _norm(x, gamma)
        k_mine = lax.dynamic_slice_in_dim(xn, z * half, half, axis=1)
        k_other = lax.dynamic_slice_in_dim(xn, (1 - z) * half, half, axis=1)
        tokens = [(k_mine, k_other), (_to(k_mine, X), _to(k_other, X))]

        own, from_y, from_z, diag = _gather([w1[:, c * c1 : (c + 1) * c1] for c in range(n1)])
        h = [[], []]
        for mine, other in ((own, from_z), (from_y, diag)):
            for core in range(2):
                for c in range(n1):
                    for t in range(2):
                        pre = _dot(tokens[t][0], mine[c][core]) + _dot(tokens[t][1], other[c][core])
                        h[t].append(jax.nn.gelu(pre, approximate=True).astype(jnp.bfloat16))

        w2, _ = lax.optimization_barrier((w2, [diag[0][0], diag[1][0]]))
        own, from_y, from_z, diag = _gather([w2[:, c * c2 : (c + 1) * c2] for c in range(n2)])
        h = lax.optimization_barrier(h)

        def partial(t, a, b, c):
            acc, i = None, 0
            for piece in (a, b):
                for core in range(2):
                    w = piece[c][core]
                    for k in range(n1):
                        p = _dot(h[t][i], w[k * c1 : (k + 1) * c1])
                        acc = p if acc is None else acc + p
                        i += 1
            return acc

        y = jnp.zeros((rows, d), jnp.bfloat16)
        for side, (a, b) in enumerate(((own, from_y), (from_z, diag))):
            for c in range(n2):
                start = lax.rem(z + side, 2) * half + c * c2
                theirs = _to(partial(1, a, b, c), X)
                h, mine = lax.optimization_barrier((h, partial(0, a, b, c)))
                xs = lax.dynamic_slice_in_dim(x, start, c2, axis=1).astype(jnp.float32)
                y = lax.dynamic_update_slice_in_dim(y, (xs + (mine + theirs)).astype(jnp.bfloat16), start, axis=1)
        return y

    return jax.shard_map(
        body,
        mesh=mesh,
        in_specs=(P(("fsdp", "tp"), None), P(None), P("fsdp", "tp"), P("tp", "fsdp")),
        out_specs=P(("fsdp", "tp"), None),
        check_vma=False,
    )
```

```python
import functools

import jax
import jax.numpy as jnp
from jax import lax
from jax.experimental import pallas as pl
from jax.experimental.pallas import tpu as pltpu
from jax.sharding import PartitionSpec as P

EPS = 1e-6
MESH = pl.DeviceIdType.MESH

ROWS, D, HALF = 1024, 4096, 2048
W = 256
NC = HALF // W
NJ = 2 * NC
BM = 512
XR = 256
LAG = 3
Y, Z, DIAG, SIB = 1, 2, 3, 4


def _kernel(x, gamma, w1, w2, y, g1, g2, xnh, xph, rbuf, h, wt, send, recv, xsend, xrecv, psend, precv, loc):
    f, t = lax.axis_index("fsdp"), lax.axis_index("tp")
    core, ix, iy = lax.rem(t, 2), lax.rem(t // 2, 2), t // 4
    to_core, to_x, to_y, to_z = (f, t + 1 - 2 * core), (f, t + 2 - 4 * ix), (f, t + 4 - 8 * iy), (1 - f, t)
    shard, got = (w1, w2), (g1, g2)
    mine, other = pl.multiple_of(f * HALF, HALF), pl.multiple_of((1 - f) * HALF, HALF)

    barrier = pltpu.get_barrier_semaphore()
    for d in (to_core, to_x, to_y, to_z):
        pl.semaphore_signal(barrier, inc=1, device_id=d, device_id_type=MESH)
    pl.semaphore_wait(barrier, 4)

    def cols(c):
        return pl.ds(pl.multiple_of(c * W, W), W)

    def copy(w, kind, src, dst_piece, c, device):
        return pltpu.make_async_remote_copy(
            src_ref=shard[w].at[:, cols(c)] if src == 0 else got[w].at[src, c],
            dst_ref=got[w].at[dst_piece, c],
            send_sem=send.at[w, kind, c],
            recv_sem=recv.at[w, dst_piece - 1, c],
            device_id=device,
            device_id_type=MESH,
        )

    def arrived(w, piece, c):
        at = got[w].at[piece, c]
        pltpu.make_async_copy(at, at, recv.at[w, piece - 1, c]).wait()

    def send_own(w, g):
        for k in range(2):
            copy(w, 0, 0, Y, 2 * g + k, to_y).start()
            copy(w, 1, 0, Z, 2 * g + 1 - k, to_z).start()
            copy(w, 2, 0, SIB, 2 * g + k, to_core).start()

    def to_sib(w, piece, c):
        copy(w, 2 + piece, piece, SIB + piece, c, to_core).start()

    def slot_a(w, g):
        arrived(w, Y, 2 * g)
        arrived(w, Z, 2 * g + 1)
        copy(w, 6, Z, DIAG, 2 * g + 1, to_y).start()
        copy(w, 6, Y, DIAG, 2 * g, to_z).start()
        if w == 0:
            send_own(*((0, g + 1) if g < 3 else (1, 0)))
        else:
            pl.when(g < 3)(lambda: send_own(1, g + 1))
        to_sib(w, Y, 2 * g)
        to_sib(w, Z, 2 * g + 1)

    def slot_b(w, g):
        arrived(w, Y, 2 * g + 1)
        arrived(w, Z, 2 * g)
        to_sib(w, Y, 2 * g + 1)
        to_sib(w, Z, 2 * g)

    def slot_c(w, g):
        arrived(w, DIAG, 2 * g)
        arrived(w, DIAG, 2 * g + 1)
        to_sib(w, DIAG, 2 * g)
        to_sib(w, DIAG, 2 * g + 1)

    send_own(0, 0)

    def x_in(i):
        return pltpu.make_async_copy(x.at[pl.ds(i * XR, XR)], h.at[pl.ds(i * XR, XR), pl.ds(0, D)], loc.at[i])

    def xn_out(i):
        return pltpu.make_async_copy(h.at[pl.ds(i * XR, XR), pl.ds(0, D)], xnh.at[pl.ds(i * XR, XR)], loc.at[4 + i])

    def xn_send(i):
        rows = pl.ds(i * XR, XR)
        return pltpu.make_async_remote_copy(
            src_ref=xnh.at[rows], dst_ref=xph.at[rows], send_sem=xsend.at[i], recv_sem=xrecv.at[i],
            device_id=to_x, device_id_type=MESH,
        )

    nx = ROWS // XR
    for i in range(nx):
        x_in(i).start()
    for i in range(nx):
        x_in(i).wait()

        def norm(b, _, i=i):
            rows = pl.ds(pl.multiple_of(i * XR + b * 16, 16), 16)
            xf = h[rows, pl.ds(0, D)].astype(jnp.float32)
            mu = jnp.mean(xf, axis=-1, keepdims=True)
            xc = xf - mu
            var = jnp.mean(jnp.square(xc), axis=-1, keepdims=True)
            h[rows, pl.ds(0, D)] = (xc * lax.rsqrt(var + EPS) * gamma[...]).astype(jnp.bfloat16)
            return 0

        lax.fori_loop(0, XR // 16, norm, 0)
        xn_out(i).start()
        if i > 0:
            xn_out(i - 1).wait()
            xn_send(i - 1).start()
    xn_out(nx - 1).wait()
    xn_send(nx - 1).start()

    def first(xn):
        def load_tokens(src, row):
            for k, at in enumerate((mine, other)):
                pltpu.make_async_copy(
                    src.at[:, pl.ds(at, HALF)], xn.at[pl.ds(row, ROWS), pl.ds(k * HALF, HALF)], loc.at[k]
                ).start()
            for k, at in enumerate((mine, other)):
                pltpu.make_async_copy(
                    src.at[:, pl.ds(at, HALF)], xn.at[pl.ds(row, ROWS), pl.ds(k * HALF, HALF)], loc.at[k]
                ).wait()

        load_tokens(xnh, 0)

        def tiles(s, c, n, row, rows, new):
            def load(q, k):
                cc, sib = c + q // 2, SIB * (q % 2)
                src = w1.at[:, cols(cc)] if (sib, k, s) == (0, 0, 0) else g1.at[sib + 2 * k + s, cc]
                return pltpu.make_async_copy(src, wt.at[q, pl.ds(k * HALF, HALF)], loc.at[2 * q + k])

            for q in range(2 * n):
                for k in range(2):
                    if new and q % 2:
                        arrived(0, SIB + 2 * k + s, c + q // 2)
                    load(q, k).start()
            nb = rows // BM

            def product(i, _):
                q, b = i // nb, lax.rem(i, nb)
                for qq in range(2 * n):

                    @pl.when(i == qq * nb)
                    def _(qq=qq):
                        for k in range(2):
                            load(qq, k).wait()

                r = pl.ds(pl.multiple_of(row + b * BM, BM), BM)
                pre = jnp.dot(xn[r, :], wt[q], preferred_element_type=jnp.float32)
                at = (lax.rem(q, 2) * 2 + s) * HALF + (c + q // 2) * W
                h[r, pl.ds(pl.multiple_of(at, W), W)] = jax.nn.gelu(pre, approximate=True).astype(jnp.bfloat16)
                return 0

            lax.fori_loop(0, 2 * n * nb, product, 0)

        for g in range(3):
            slot_a(0, g)
            tiles(0, 2 * g + 1, 1, 0, ROWS, True)
            slot_b(0, g)
            tiles(0, 2 * g, 1, 0, ROWS, True)
            if g < 2:
                slot_c(0, g)
                tiles(1, 2 * g, 2, 0, ROWS, True)
        for i in range(nx):
            xn_send(i).wait_recv()
        load_tokens(xph, ROWS)
        for s in range(2):
            tiles(s, 0, 2, ROWS, ROWS, False)
        slot_c(0, 2)
        for s in range(2):
            tiles(s, 2, 2, ROWS, ROWS, False)
        tiles(1, 4, 2, 0, 2 * ROWS, True)
        slot_a(0, 3)
        tiles(0, 4, 2, ROWS, ROWS, False)
        tiles(0, 7, 1, 0, 2 * ROWS, True)
        slot_b(0, 3)
        tiles(0, 6, 1, 0, 2 * ROWS, True)
        slot_c(0, 3)
        tiles(1, 6, 2, 0, 2 * ROWS, True)

    pl.run_scoped(first, pltpu.VMEM((2 * ROWS, D), jnp.bfloat16))

    def second(theirs, own, back, xb, yb):
        def where(j):
            r, c = lax.rem(j, 4) // 2, 2 * (j // 4) + lax.rem(j, 2)
            return r, c, pl.multiple_of(lax.rem(f + r, 2) * HALF + c * W, W)

        def partial_out(j):
            return pltpu.make_async_remote_copy(
                src_ref=theirs.at[lax.rem(j, LAG)], dst_ref=rbuf.at[j], send_sem=psend.at[j], recv_sem=precv.at[j],
                device_id=to_x, device_id_type=MESH,
            )

        def y_out(j):
            _, _, at = where(j)
            return pltpu.make_async_copy(yb.at[lax.rem(j, 2)], y.at[:, pl.ds(at, W)], loc.at[6 + lax.rem(j, 2)])

        def finish(j):
            _, _, at = where(j)
            a = pltpu.make_async_copy(x.at[:, pl.ds(at, W)], xb, loc.at[4])
            b = pltpu.make_async_copy(rbuf.at[j], back, loc.at[5])
            a.start()
            partial_out(j).wait_recv()
            b.start()
            pl.when(j >= 2)(lambda: y_out(j - 2).wait())
            a.wait()
            b.wait()

            def add(i, _):
                r = pl.ds(pl.multiple_of(i * 64, 64), 64)
                total = own[lax.rem(j, LAG + 1), r, :] + back[r, :]
                yb[lax.rem(j, 2), r, :] = (xb[r, :].astype(jnp.float32) + total).astype(jnp.bfloat16)
                return 0

            lax.fori_loop(0, ROWS // 64, add, 0)
            y_out(j).start()

        def product(row, b):
            r = pl.ds(pl.multiple_of(row + b * BM, BM), BM)
            return sum(
                jnp.dot(h[r, pl.ds(k * D, D)], wt[k], preferred_element_type=jnp.float32) for k in range(2)
            )

        def chunk(j, _):
            g, q = j // 4, lax.rem(j, 4)
            r, c, _ = where(j)
            pl.when(q == 0)(lambda: slot_a(1, g))
            pl.when(q == 1)(lambda: slot_b(1, g))
            pl.when(q == 2)(lambda: slot_c(1, g))

            def load(sib, s):
                src = g2.at[SIB * sib + 2 * r + s, c]
                return pltpu.make_async_copy(src, wt.at[sib, pl.ds(s * HALF, HALF)], loc.at[2 * sib + s])

            @pl.when(r == 0)
            def _():
                pltpu.make_async_copy(w2.at[:, cols(c)], wt.at[0, pl.ds(0, HALF)], loc.at[0]).start()

            @pl.when(r == 1)
            def _():
                load(0, 0).start()

            load(0, 1).start()
            for s in range(2):
                arrived(1, SIB + 2 * r + s, c)
                load(1, s).start()
            pl.when(j >= LAG)(lambda: partial_out(j - LAG).wait_send())
            for sib in range(2):
                for s in range(2):
                    load(sib, s).wait()

            def to_them(b, _):
                theirs[lax.rem(j, LAG), pl.ds(pl.multiple_of(b * BM, BM), BM), :] = product(ROWS, b)
                return 0

            lax.fori_loop(0, ROWS // BM, to_them, 0)
            partial_out(j).start()

            def to_us(b, _):
                own[lax.rem(j, LAG + 1), pl.ds(pl.multiple_of(b * BM, BM), BM), :] = product(0, b)
                return 0

            lax.fori_loop(0, ROWS // BM, to_us, 0)
            pl.when(j >= LAG)(lambda: finish(j - LAG))
            return 0

        lax.fori_loop(0, NJ, chunk, 0)

        def drain(j, _):
            finish(j)
            partial_out(j).wait_send()
            return 0

        lax.fori_loop(NJ - LAG, NJ, drain, 0)
        for j in range(NJ - 2, NJ):
            y_out(j).wait()

    pl.run_scoped(
        second,
        pltpu.VMEM((LAG, ROWS, W), jnp.float32),
        pltpu.VMEM((LAG + 1, ROWS, W), jnp.float32),
        pltpu.VMEM((ROWS, W), jnp.float32),
        pltpu.VMEM((ROWS, W), jnp.bfloat16),
        pltpu.VMEM((2, ROWS, W), jnp.bfloat16),
    )

    for i in range(nx):
        xn_send(i).wait_send()

    def sent(c, _):
        for w in range(2):
            for kind in range(7):
                copy(w, kind, Y, Y, c, to_y).wait_send()
        return 0

    lax.fori_loop(0, NC, sent, 0)


def solution(mesh):
    hbm = pl.BlockSpec(memory_space=pltpu.HBM)
    vmem = pl.BlockSpec(memory_space=pltpu.VMEM)

    def body(x, gamma, w1, w2):
        bf16 = functools.partial(jax.ShapeDtypeStruct, dtype=jnp.bfloat16)
        out = pl.pallas_call(
            _kernel,
            out_shape=[
                bf16((ROWS, D)),
                bf16((8, NC, HALF, W)),
                bf16((8, NC, HALF, W)),
                bf16((ROWS, D)),
                bf16((ROWS, D)),
                jax.ShapeDtypeStruct((NJ, ROWS, W), jnp.float32),
            ],
            in_specs=[hbm, vmem, hbm, hbm],
            out_specs=[hbm] * 6,
            scratch_shapes=[
                pltpu.VMEM((2 * ROWS, 4 * HALF), jnp.bfloat16),
                pltpu.VMEM((4, D, W), jnp.bfloat16),
                pltpu.SemaphoreType.DMA((2, 7, NC)),
                pltpu.SemaphoreType.DMA((2, 7, NC)),
                pltpu.SemaphoreType.DMA((ROWS // XR,)),
                pltpu.SemaphoreType.DMA((ROWS // XR,)),
                pltpu.SemaphoreType.DMA((NJ,)),
                pltpu.SemaphoreType.DMA((NJ,)),
                pltpu.SemaphoreType.DMA((8,)),
            ],
            compiler_params=pltpu.CompilerParams(
                collective_id=0, has_side_effects=True, vmem_limit_bytes=67_043_328
            ),
            cost_estimate=pl.CostEstimate(flops=275_000_000_000, bytes_accessed=400_000_000, transcendentals=16_777_216),
        )(x, gamma.reshape(1, D), w1, w2)
        return out[0]

    return jax.shard_map(
        body,
        mesh=mesh,
        in_specs=(P(("fsdp", "tp"), None), P(None), P("fsdp", "tp"), P("tp", "fsdp")),
        out_specs=P(("fsdp", "tp"), None),
        check_vma=False,
    )
```

```python
import functools

import jax
import jax.numpy as jnp
from jax import lax
from jax.experimental import pallas as pl
from jax.experimental.pallas import tpu as pltpu
from jax.sharding import PartitionSpec as P

EPS = 1e-6
MESH = pl.DeviceIdType.MESH

ROWS, D, HALF = 1024, 4096, 2048
W = 256
NC = HALF // W
NJ = 2 * NC
BM = 512
XR = 256
LAG = 3
Y, Z, DIAG, SIB = 1, 2, 3, 4


def _kernel(x, gamma, w1, w2, y, g1, g2, xnh, xph, rbuf, h, wt, send, recv, xsend, xrecv, psend, precv, loc):
    f, t = lax.axis_index("fsdp"), lax.axis_index("tp")
    core, ix, iy = lax.rem(t, 2), lax.rem(t // 2, 2), t // 4
    to_core, to_x, to_y, to_z = (f, t + 1 - 2 * core), (f, t + 2 - 4 * ix), (f, t + 4 - 8 * iy), (1 - f, t)
    shard, got = (w1, w2), (g1, g2)
    mine, other = pl.multiple_of(f * HALF, HALF), pl.multiple_of((1 - f) * HALF, HALF)

    barrier = pltpu.get_barrier_semaphore()
    for d in (to_core, to_x, to_y, to_z):
        pl.semaphore_signal(barrier, inc=1, device_id=d, device_id_type=MESH)
    pl.semaphore_wait(barrier, 4)

    def cols(c):
        return pl.ds(pl.multiple_of(c * W, W), W)

    def copy(w, kind, src, dst_piece, c, device):
        return pltpu.make_async_remote_copy(
            src_ref=shard[w].at[:, cols(c)] if src == 0 else got[w].at[src, c],
            dst_ref=got[w].at[dst_piece, c],
            send_sem=send.at[w, kind, c],
            recv_sem=recv.at[w, dst_piece - 1, c],
            device_id=device,
            device_id_type=MESH,
        )

    def arrived(w, piece, c):
        at = got[w].at[piece, c]
        pltpu.make_async_copy(at, at, recv.at[w, piece - 1, c]).wait()

    def send_own(w, g):
        for k in range(2):
            copy(w, 0, 0, Y, 2 * g + k, to_y).start()
            copy(w, 1, 0, Z, 2 * g + 1 - k, to_z).start()
            copy(w, 2, 0, SIB, 2 * g + k, to_core).start()

    def to_sib(w, piece, c):
        copy(w, 2 + piece, piece, SIB + piece, c, to_core).start()

    def slot_a(w, g):
        arrived(w, Y, 2 * g)
        arrived(w, Z, 2 * g + 1)
        copy(w, 6, Z, DIAG, 2 * g + 1, to_y).start()
        copy(w, 6, Y, DIAG, 2 * g, to_z).start()
        if w == 0:
            send_own(*((0, g + 1) if g < 3 else (1, 0)))
        else:
            pl.when(g < 3)(lambda: send_own(1, g + 1))
        to_sib(w, Y, 2 * g)
        to_sib(w, Z, 2 * g + 1)

    def slot_b(w, g):
        arrived(w, Y, 2 * g + 1)
        arrived(w, Z, 2 * g)
        to_sib(w, Y, 2 * g + 1)
        to_sib(w, Z, 2 * g)

    def slot_c(w, g):
        arrived(w, DIAG, 2 * g)
        arrived(w, DIAG, 2 * g + 1)
        to_sib(w, DIAG, 2 * g)
        to_sib(w, DIAG, 2 * g + 1)

    send_own(0, 0)

    def x_in(i):
        return pltpu.make_async_copy(x.at[pl.ds(i * XR, XR)], h.at[pl.ds(i * XR, XR), pl.ds(0, D)], loc.at[i])

    def xn_out(i):
        return pltpu.make_async_copy(h.at[pl.ds(i * XR, XR), pl.ds(0, D)], xnh.at[pl.ds(i * XR, XR)], loc.at[4 + i])

    def xn_send(i):
        rows = pl.ds(i * XR, XR)
        return pltpu.make_async_remote_copy(
            src_ref=xnh.at[rows], dst_ref=xph.at[rows], send_sem=xsend.at[i], recv_sem=xrecv.at[i],
            device_id=to_x, device_id_type=MESH,
        )

    nx = ROWS // XR
    for i in range(nx):
        x_in(i).start()
    for i in range(nx):
        x_in(i).wait()

        def norm(b, _, i=i):
            rows = pl.ds(pl.multiple_of(i * XR + b * 16, 16), 16)
            xf = h[rows, pl.ds(0, D)].astype(jnp.float32)
            mu = jnp.mean(xf, axis=-1, keepdims=True)
            xc = xf - mu
            var = jnp.mean(jnp.square(xc), axis=-1, keepdims=True)
            h[rows, pl.ds(0, D)] = (xc * lax.rsqrt(var + EPS) * gamma[...]).astype(jnp.bfloat16)
            return 0

        lax.fori_loop(0, XR // 16, norm, 0)
        xn_out(i).start()
        if i > 0:
            xn_out(i - 1).wait()
            xn_send(i - 1).start()
    xn_out(nx - 1).wait()
    xn_send(nx - 1).start()

    def first(xn, pre):
        def load_tokens(src, at, row, rows):
            def part(k, column):
                return pltpu.make_async_copy(
                    src.at[pl.ds(at, rows), pl.ds(column, HALF)],
                    xn.at[pl.ds(row, rows), pl.ds(k * HALF, HALF)],
                    loc.at[k],
                )

            for k, column in enumerate((mine, other)):
                part(k, column).start()
            for k, column in enumerate((mine, other)):
                part(k, column).wait()

        def load(unit, slot, q, wait):
            s, by_core, c, core = unit
            cc, cr = c + by_core * q, (1 - by_core) * q + by_core * core

            def start(src, k):
                pltpu.make_async_copy(src, wt.at[slot, pl.ds(k * HALF, HALF)], loc.at[2 * slot + k]).start()

            @pl.when((cr == 0) & (s == 0))
            def _():
                start(w1.at[:, cols(cc)], 0)

            @pl.when((cr == 0) & (s == 1))
            def _():
                start(g1.at[Y, cc], 0)

            @pl.when(cr == 0)
            def _():
                start(g1.at[Z + s, cc], 1)

            @pl.when(cr == 1)
            def _():
                for k in range(2):

                    @pl.when(wait)
                    def _(k=k):
                        arrived(0, SIB + 2 * k + s, cc)

                    start(g1.at[SIB + 2 * k + s, cc], k)

        def store_last(last):
            row, column = last
            at = pl.ds(pl.multiple_of(row, BM), BM), pl.ds(pl.multiple_of(column, W), W)
            h[at] = jax.nn.gelu(pre[...], approximate=True).astype(jnp.bfloat16)

        def run(n, unit, rows, ready, wait, last, ahead=lambda i: 0):
            def load_unit(i):
                ready(i)
                for q in range(2):
                    load(unit(i), 2 * lax.rem(i, 2) + q, q, wait(i))

            def one(i, last):
                pl.when((i == 0) | (i * 0 + ahead(i) < 0))(lambda: load_unit(i))
                s, by_core, c, core = unit(i)
                b0, nb = rows(i)

                def product(m, last):
                    q, b = m // nb, lax.rem(m, nb)
                    slot = 2 * lax.rem(i, 2) + q

                    @pl.when(b == 0)
                    def _():
                        for k in range(2):
                            pltpu.make_async_copy(
                                g1.at[Y, 0], wt.at[slot, pl.ds(k * HALF, HALF)], loc.at[2 * slot + k]
                            ).wait()

                    pl.when((i + 1 < n) & (m == ahead(i + 1)))(lambda: load_unit(i + 1))
                    row = (b0 + b) * BM
                    column = (((1 - by_core) * q + by_core * core) * 2 + s) * HALF + (c + by_core * q) * W
                    store_last(last)
                    r = pl.ds(pl.multiple_of(row, BM), BM)
                    pre[...] = jnp.dot(xn[r, :], wt[slot], preferred_element_type=jnp.float32)
                    return row, column

                return lax.fori_loop(0, 2 * nb, product, last)

            return lax.fori_loop(0, n, one, last)

        load_tokens(xnh, 0, 0, ROWS)
        zero = lax.rem(core, 1)
        last = (zero, zero + W)
        yes, no = (lambda i: i >= 0), (lambda i: i < 0)
        nothing = lambda i: None

        slot_a(0, 0)
        last = run(1, lambda i: (0, 0, 1, 0), lambda i: (0, 2), nothing, yes, last)
        slot_b(0, 0)
        last = run(1, lambda i: (0, 0, 0, 0), lambda i: (0, 2), nothing, yes, last)
        slot_c(0, 0)
        last = run(2, lambda i: (1, 1, 0, i), lambda i: (0, 2), nothing, yes, last, lambda i: 2)
        slot_a(0, 1)
        last = run(1, lambda i: (0, 0, 3, 0), lambda i: (0, 2), nothing, yes, last)
        for i in range(nx // 2):
            xn_send(i).wait_recv()
        load_tokens(xph, 0, ROWS, ROWS // 2)
        last = run(4, lambda i: (i // 2, 0, lax.rem(i, 2), 0), lambda i: (2, 1), nothing, no, last)
        slot_b(0, 1)
        last = run(1, lambda i: (0, 0, 2, 0), lambda i: (0, 3), nothing, yes, last)
        last = run(1, lambda i: (0, 0, 3, 0), lambda i: (2, 1), nothing, no, last)
        slot_c(0, 1)
        last = run(2, lambda i: (1, 1, 2, i), lambda i: (0, 3), nothing, yes, last, lambda i: 3)
        slot_a(0, 2)
        last = run(1, lambda i: (0, 0, 5, 0), lambda i: (0, 3), nothing, yes, last)
        slot_b(0, 2)
        last = run(1, lambda i: (0, 0, 4, 0), lambda i: (0, 3), nothing, yes, last)
        for i in range(nx // 2, nx):
            xn_send(i).wait_recv()
        load_tokens(xph, ROWS // 2, ROWS + ROWS // 2, ROWS // 2)

        def unit(i):
            late = i >= 10
            s = jnp.where(late, jnp.where((i == 12) | (i == 13), 0, 1), lax.rem(i // 2, 2))
            s = jnp.where((i == 8) | (i == 9), 0, s)
            by_core = jnp.where(late & (s == 1), 1, 0)
            c = jnp.where(i < 8, 2 * (i // 4) + lax.rem(i, 2), i - 4)
            c = jnp.where(i >= 10, 4, c)
            c = jnp.where(i == 12, 7, c)
            c = jnp.where(i >= 13, 6, c)
            return s, by_core, c, lax.rem(i, 2)

        def rows(i):
            return jnp.where(i >= 10, 0, 3), jnp.where(i >= 10, 4, 1)

        def ready(i):
            pl.when(i == 10)(lambda: slot_c(0, 2))
            pl.when(i == 12)(lambda: slot_a(0, 3))
            pl.when(i == 13)(lambda: slot_b(0, 3))
            pl.when(i == 14)(lambda: slot_c(0, 3))

        def ahead(i):
            return jnp.where(i < 12, 0, jnp.where((i == 12) | (i == 15), 4, -1))

        last = run(16, unit, rows, ready, lambda i: i >= 10, last, ahead)
        store_last(last)

    pl.run_scoped(first, pltpu.VMEM((2 * ROWS, D), jnp.bfloat16), pltpu.VMEM((BM, W), jnp.float32))

    def second(theirs, own, back, xb, yb):
        def where(j):
            r, c = lax.rem(j, 4) // 2, 2 * (j // 4) + lax.rem(j, 2)
            return r, c, pl.multiple_of(lax.rem(f + r, 2) * HALF + c * W, W)

        def partial_out(j):
            return pltpu.make_async_remote_copy(
                src_ref=theirs.at[lax.rem(j, LAG)], dst_ref=rbuf.at[j], send_sem=psend.at[j], recv_sem=precv.at[j],
                device_id=to_x, device_id_type=MESH,
            )

        def y_out(j):
            _, _, at = where(j)
            return pltpu.make_async_copy(yb.at[lax.rem(j, 2)], y.at[:, pl.ds(at, W)], loc.at[6 + lax.rem(j, 2)])

        def finish(j):
            _, _, at = where(j)
            a = pltpu.make_async_copy(x.at[:, pl.ds(at, W)], xb, loc.at[4])
            b = pltpu.make_async_copy(rbuf.at[j], back, loc.at[5])
            a.start()
            partial_out(j).wait_recv()
            b.start()
            pl.when(j >= 2)(lambda: y_out(j - 2).wait())
            a.wait()
            b.wait()

            def add(i, _):
                r = pl.ds(pl.multiple_of(i * 64, 64), 64)
                total = own[lax.rem(j, LAG + 1), r, :] + back[r, :]
                yb[lax.rem(j, 2), r, :] = (xb[r, :].astype(jnp.float32) + total).astype(jnp.bfloat16)
                return 0

            lax.fori_loop(0, ROWS // 64, add, 0)
            y_out(j).start()

        def product(row, b):
            r = pl.ds(pl.multiple_of(row + b * BM, BM), BM)
            return sum(
                jnp.dot(h[r, pl.ds(k * D, D)], wt[k], preferred_element_type=jnp.float32) for k in range(2)
            )

        def chunk(j, _):
            g, q = j // 4, lax.rem(j, 4)
            r, c, _ = where(j)
            pl.when(q == 0)(lambda: slot_a(1, g))
            pl.when(q == 1)(lambda: slot_b(1, g))
            pl.when(q == 2)(lambda: slot_c(1, g))

            def load(sib, s):
                src = g2.at[SIB * sib + 2 * r + s, c]
                return pltpu.make_async_copy(src, wt.at[sib, pl.ds(s * HALF, HALF)], loc.at[2 * sib + s])

            @pl.when(r == 0)
            def _():
                pltpu.make_async_copy(w2.at[:, cols(c)], wt.at[0, pl.ds(0, HALF)], loc.at[0]).start()

            @pl.when(r == 1)
            def _():
                load(0, 0).start()

            load(0, 1).start()
            for s in range(2):
                arrived(1, SIB + 2 * r + s, c)
                load(1, s).start()
            pl.when(j >= LAG)(lambda: partial_out(j - LAG).wait_send())
            for sib in range(2):
                for s in range(2):
                    load(sib, s).wait()

            def to_them(b, _):
                theirs[lax.rem(j, LAG), pl.ds(pl.multiple_of(b * BM, BM), BM), :] = product(ROWS, b)
                return 0

            lax.fori_loop(0, ROWS // BM, to_them, 0)
            partial_out(j).start()

            def to_us(b, _):
                own[lax.rem(j, LAG + 1), pl.ds(pl.multiple_of(b * BM, BM), BM), :] = product(0, b)
                return 0

            lax.fori_loop(0, ROWS // BM, to_us, 0)
            pl.when(j >= LAG)(lambda: finish(j - LAG))
            return 0

        lax.fori_loop(0, NJ, chunk, 0)

        def drain(j, _):
            finish(j)
            partial_out(j).wait_send()
            return 0

        lax.fori_loop(NJ - LAG, NJ, drain, 0)
        for j in range(NJ - 2, NJ):
            y_out(j).wait()

    pl.run_scoped(
        second,
        pltpu.VMEM((LAG, ROWS, W), jnp.float32),
        pltpu.VMEM((LAG + 1, ROWS, W), jnp.float32),
        pltpu.VMEM((ROWS, W), jnp.float32),
        pltpu.VMEM((ROWS, W), jnp.bfloat16),
        pltpu.VMEM((2, ROWS, W), jnp.bfloat16),
    )

    for i in range(nx):
        xn_send(i).wait_send()

    def sent(c, _):
        for w in range(2):
            for kind in range(7):
                copy(w, kind, Y, Y, c, to_y).wait_send()
        return 0

    lax.fori_loop(0, NC, sent, 0)


def solution(mesh):
    hbm = pl.BlockSpec(memory_space=pltpu.HBM)
    vmem = pl.BlockSpec(memory_space=pltpu.VMEM)

    def body(x, gamma, w1, w2):
        bf16 = functools.partial(jax.ShapeDtypeStruct, dtype=jnp.bfloat16)
        out = pl.pallas_call(
            _kernel,
            out_shape=[
                bf16((ROWS, D)),
                bf16((8, NC, HALF, W)),
                bf16((8, NC, HALF, W)),
                bf16((ROWS, D)),
                bf16((ROWS, D)),
                jax.ShapeDtypeStruct((NJ, ROWS, W), jnp.float32),
            ],
            in_specs=[hbm, vmem, hbm, hbm],
            out_specs=[hbm] * 6,
            scratch_shapes=[
                pltpu.VMEM((2 * ROWS, 4 * HALF), jnp.bfloat16),
                pltpu.VMEM((4, D, W), jnp.bfloat16),
                pltpu.SemaphoreType.DMA((2, 7, NC)),
                pltpu.SemaphoreType.DMA((2, 7, NC)),
                pltpu.SemaphoreType.DMA((ROWS // XR,)),
                pltpu.SemaphoreType.DMA((ROWS // XR,)),
                pltpu.SemaphoreType.DMA((NJ,)),
                pltpu.SemaphoreType.DMA((NJ,)),
                pltpu.SemaphoreType.DMA((8,)),
            ],
            compiler_params=pltpu.CompilerParams(
                collective_id=0, has_side_effects=True, vmem_limit_bytes=67_043_328
            ),
            cost_estimate=pl.CostEstimate(flops=275_000_000_000, bytes_accessed=400_000_000, transcendentals=16_777_216),
        )(x, gamma.reshape(1, D), w1, w2)
        return out[0]

    return jax.shard_map(
        body,
        mesh=mesh,
        in_specs=(P(("fsdp", "tp"), None), P(None), P("fsdp", "tp"), P("tp", "fsdp")),
        out_specs=P(("fsdp", "tp"), None),
        check_vma=False,
    )
```

```python
import functools

import jax
import jax.numpy as jnp
from jax import lax
from jax.experimental import pallas as pl
from jax.experimental.pallas import tpu as pltpu
from jax.sharding import PartitionSpec as P

EPS = 1e-6
MESH = pl.DeviceIdType.MESH

ROWS, D, HALF = 1024, 4096, 2048
W = 256
NC = HALF // W
NJ = 2 * NC
BM = 512
XR = 256
LAG = 3
SLOTS = 2
Y, Z, DIAG, SIB = 1, 2, 3, 4


def _kernel(x, gamma, w1, w2, y, g1, g2, xnh, xph, rbuf, h, wt, send, recv, xsend, xrecv, psend, precv, ysend, yrecv, loc):
    f, t = lax.axis_index("fsdp"), lax.axis_index("tp")
    core, ix, iy = lax.rem(t, 2), lax.rem(t // 2, 2), t // 4
    to_core, to_x, to_y, to_z = (f, t + 1 - 2 * core), (f, t + 2 - 4 * ix), (f, t + 4 - 8 * iy), (1 - f, t)
    shard, got = (w1, w2), (g1, g2)
    mine, other = pl.multiple_of(f * HALF, HALF), pl.multiple_of((1 - f) * HALF, HALF)

    barrier = pltpu.get_barrier_semaphore()
    for d in (to_core, to_x, to_y, to_z):
        pl.semaphore_signal(barrier, inc=1, device_id=d, device_id_type=MESH)
    pl.semaphore_wait(barrier, 4)

    def cols(c):
        return pl.ds(pl.multiple_of(c * W, W), W)

    def copy(w, kind, src, dst_piece, c, device):
        return pltpu.make_async_remote_copy(
            src_ref=shard[w].at[:, cols(c)] if src == 0 else got[w].at[src, c],
            dst_ref=got[w].at[dst_piece, c],
            send_sem=send.at[w, kind, c],
            recv_sem=recv.at[w, dst_piece - 1, c],
            device_id=device,
            device_id_type=MESH,
        )

    def arrived(w, piece, c):
        at = got[w].at[piece, c]
        pltpu.make_async_copy(at, at, recv.at[w, piece - 1, c]).wait()

    def half_cols(u):
        return pl.ds(u * (W // 2), W // 2)

    def y_half(u):
        return pltpu.make_async_remote_copy(
            src_ref=w2.at[:, half_cols(u)], dst_ref=g2.at[Y, 0, :, half_cols(u)], send_sem=ysend.at[u],
            recv_sem=yrecv.at[u], device_id=to_y, device_id_type=MESH,
        )

    def y_half_to_sib(u):
        return pltpu.make_async_remote_copy(
            src_ref=g2.at[Y, 0, :, half_cols(u)], dst_ref=g2.at[SIB + Y, 0, :, half_cols(u)], send_sem=ysend.at[2 + u],
            recv_sem=yrecv.at[2 + u], device_id=to_core, device_id_type=MESH,
        )

    def send_own(w, g):
        for k in range(2):
            if w == 1 and k == 0 and isinstance(g, int):
                y_half(0).start()
                y_half(1).start()
            else:
                copy(w, 0, 0, Y, 2 * g + k, to_y).start()
            copy(w, 1, 0, Z, 2 * g + 1 - k, to_z).start()
            copy(w, 2, 0, SIB, 2 * g + k, to_core).start()

    def to_sib(w, piece, c):
        copy(w, 2 + piece, piece, SIB + piece, c, to_core).start()

    def slot_a(w, g, halves=False):
        if not halves:
            arrived(w, Y, 2 * g)
        arrived(w, Z, 2 * g + 1)
        copy(w, 6, Z, DIAG, 2 * g + 1, to_y).start()
        copy(w, 6, Y, DIAG, 2 * g, to_z).start()
        if w == 0:
            send_own(*((0, g + 1) if g < 3 else (1, 0)))
        else:
            pl.when(g < 3)(lambda: send_own(1, g + 1 + core * 0))
        if not halves:
            to_sib(w, Y, 2 * g)
        to_sib(w, Z, 2 * g + 1)

    def slot_b(w, g):
        arrived(w, Y, 2 * g + 1)
        arrived(w, Z, 2 * g)
        to_sib(w, Y, 2 * g + 1)
        to_sib(w, Z, 2 * g)

    def slot_c(w, g):
        arrived(w, DIAG, 2 * g)
        arrived(w, DIAG, 2 * g + 1)
        to_sib(w, DIAG, 2 * g)
        to_sib(w, DIAG, 2 * g + 1)

    send_own(0, 0)

    def x_in(i):
        return pltpu.make_async_copy(x.at[pl.ds(i * XR, XR)], h.at[pl.ds(i * XR, XR), pl.ds(0, D)], loc.at[i])

    def xn_out(i):
        return pltpu.make_async_copy(h.at[pl.ds(i * XR, XR), pl.ds(0, D)], xnh.at[pl.ds(i * XR, XR)], loc.at[4 + i])

    def xn_send(i):
        rows = pl.ds(i * XR, XR)
        return pltpu.make_async_remote_copy(
            src_ref=xnh.at[rows], dst_ref=xph.at[rows], send_sem=xsend.at[i], recv_sem=xrecv.at[i],
            device_id=to_x, device_id_type=MESH,
        )

    nx = ROWS // XR
    for i in range(nx):
        x_in(i).start()
    for i in range(nx):
        x_in(i).wait()

        def norm(b, _, i=i):
            rows = pl.ds(pl.multiple_of(i * XR + b * 16, 16), 16)
            xf = h[rows, pl.ds(0, D)].astype(jnp.float32)
            mu = jnp.mean(xf, axis=-1, keepdims=True)
            xc = xf - mu
            var = jnp.mean(jnp.square(xc), axis=-1, keepdims=True)
            h[rows, pl.ds(0, D)] = (xc * lax.rsqrt(var + EPS) * gamma[...]).astype(jnp.bfloat16)
            return 0

        lax.fori_loop(0, XR // 16, norm, 0)
        xn_out(i).start()
        if i > 0:
            xn_out(i - 1).wait()
            xn_send(i - 1).start()
    xn_out(nx - 1).wait()
    xn_send(nx - 1).start()

    def first(xn, pre, theirs):
        def load_tokens(src, at, row, rows):
            def part(k, column):
                return pltpu.make_async_copy(
                    src.at[pl.ds(at, rows), pl.ds(column, HALF)],
                    xn.at[pl.ds(row, rows), pl.ds(k * HALF, HALF)],
                    loc.at[k],
                )

            for k, column in enumerate((mine, other)):
                part(k, column).start()
            for k, column in enumerate((mine, other)):
                part(k, column).wait()

        def load(unit, slot, q, wait):
            s, by_core, c, core = unit
            cc, cr = c + by_core * q, (1 - by_core) * q + by_core * core

            def start(src, k):
                pltpu.make_async_copy(src, wt.at[slot, pl.ds(k * HALF, HALF)], loc.at[2 * slot + k]).start()

            @pl.when((cr == 0) & (s == 0))
            def _():
                start(w1.at[:, cols(cc)], 0)

            @pl.when((cr == 0) & (s == 1))
            def _():
                start(g1.at[Y, cc], 0)

            @pl.when(cr == 0)
            def _():
                start(g1.at[Z + s, cc], 1)

            @pl.when(cr == 1)
            def _():
                for k in range(2):

                    @pl.when(wait)
                    def _(k=k):
                        arrived(0, SIB + 2 * k + s, cc)

                    start(g1.at[SIB + 2 * k + s, cc], k)

        def store_last(last):
            row, column = last
            at = pl.ds(pl.multiple_of(row, BM), BM), pl.ds(pl.multiple_of(column, W), W)
            h[at] = jax.nn.gelu(pre[...], approximate=True).astype(jnp.bfloat16)

        def run(n, unit, rows, ready, wait, last, ahead=lambda i: 0):
            def load_unit(i):
                ready(i)
                for q in range(2):
                    load(unit(i), 2 * lax.rem(i, 2) + q, q, wait(i))

            def one(i, last):
                pl.when((i == 0) | (i * 0 + ahead(i) < 0))(lambda: load_unit(i))
                hook = lambda m: pl.when((i + 1 < n) & (m == ahead(i + 1)))(lambda: load_unit(i + 1))
                return products(unit(i), 2 * lax.rem(i, 2), rows(i), last, hook)

            return lax.fori_loop(0, n, one, last)

        def products(unit, slot0, rows, last, hook=None):
                s, by_core, c, core = unit
                b0, nb = rows

                def product(m, last):
                    q, b = m // nb, lax.rem(m, nb)
                    slot = slot0 + q

                    @pl.when((b == 0) & (hook is not None))
                    def _():
                        for k in range(2):
                            pltpu.make_async_copy(
                                g1.at[Y, 0], wt.at[slot, pl.ds(k * HALF, HALF)], loc.at[2 * slot + k]
                            ).wait()

                    if hook is not None:
                        hook(m)
                    row = (b0 + b) * BM
                    column = (((1 - by_core) * q + by_core * core) * 2 + s) * HALF + (c + by_core * q) * W
                    store_last(last)
                    r = pl.ds(pl.multiple_of(row, BM), BM)
                    pre[...] = jnp.dot(xn[r, :], wt[slot], preferred_element_type=jnp.float32)
                    return row, column

                return lax.fori_loop(0, 2 * nb, product, last)

        load_tokens(xnh, 0, 0, ROWS)
        zero = lax.rem(core, 1)
        last = (zero, zero + W)
        yes, no = (lambda i: i >= 0), (lambda i: i < 0)
        nothing = lambda i: None

        slot_a(0, 0)
        last = run(1, lambda i: (0, 0, 1, 0), lambda i: (0, 2), nothing, yes, last)
        slot_b(0, 0)
        last = run(1, lambda i: (0, 0, 0, 0), lambda i: (0, 2), nothing, yes, last)
        slot_c(0, 0)
        last = run(2, lambda i: (1, 1, 0, i), lambda i: (0, 2), nothing, yes, last, lambda i: 2)
        slot_a(0, 1)
        last = run(1, lambda i: (0, 0, 3, 0), lambda i: (0, 2), nothing, yes, last)
        for i in range(nx // 2):
            xn_send(i).wait_recv()
        load_tokens(xph, 0, ROWS, ROWS // 2)
        last = run(4, lambda i: (i // 2, 0, lax.rem(i, 2), 0), lambda i: (2, 1), nothing, no, last)
        slot_b(0, 1)
        last = run(1, lambda i: (0, 0, 2, 0), lambda i: (0, 3), nothing, yes, last)
        last = run(1, lambda i: (0, 0, 3, 0), lambda i: (2, 1), nothing, no, last)
        slot_c(0, 1)
        last = run(2, lambda i: (1, 1, 2, i), lambda i: (0, 3), nothing, yes, last, lambda i: 3)
        slot_a(0, 2)
        last = run(1, lambda i: (0, 0, 5, 0), lambda i: (0, 3), nothing, yes, last)
        slot_b(0, 2)
        last = run(1, lambda i: (0, 0, 4, 0), lambda i: (0, 3), nothing, yes, last)
        for i in range(nx // 2, nx):
            xn_send(i).wait_recv()
        load_tokens(xph, ROWS // 2, ROWS + ROWS // 2, ROWS // 2)

        def unit(i):
            late = i >= 10
            s = jnp.where(late, jnp.where((i == 12) | (i == 13), 0, 1), lax.rem(i // 2, 2))
            s = jnp.where((i == 8) | (i == 9), 0, s)
            by_core = jnp.where(late & (s == 1), 1, 0)
            c = jnp.where(i < 8, 2 * (i // 4) + lax.rem(i, 2), i - 4)
            c = jnp.where(i >= 10, 4, c)
            c = jnp.where(i == 12, 7, c)
            c = jnp.where(i >= 13, 6, c)
            return s, by_core, c, lax.rem(i, 2)

        def rows(i):
            return jnp.where(i >= 10, jnp.where(i >= 14, 2, 0), 3), jnp.where(i >= 10, jnp.where(i >= 14, 2, 4), 1)

        def ready(i):
            pl.when(i == 10)(lambda: slot_c(0, 2))
            pl.when(i == 12)(lambda: slot_a(0, 3))
            pl.when(i == 13)(lambda: slot_b(0, 3))
            pl.when(i == 14)(lambda: slot_c(0, 3))

        def ahead(i):
            return jnp.where(i < 12, 0, jnp.where(i == 12, 4, jnp.where(i == 15, 2, -1)))

        last = run(16, unit, rows, ready, lambda i: i >= 10, last, ahead)

        for u in range(2):
            last = products((1, 1, 6, u), 2 * u, (0, 2), last)
            store_last(last)
            y_half(u).wait_recv()
            y_half_to_sib(u).start()
            pieces = (w2, g2.at[Y, 0], g2.at[SIB, 0], g2.at[SIB + Y, 0])
            if u == 0:
                arrived(1, SIB, 0)

            def load_half(i, u=u):
                src = w2.at[:, half_cols(u)] if i == 0 else pieces[i].at[:, half_cols(u)]
                return pltpu.make_async_copy(
                    src, wt.at[i // 2, pl.ds(i % 2 * HALF, HALF), half_cols(u)], loc.at[i]
                )

            for i in range(3):
                load_half(i).start()
            y_half_to_sib(u).wait_recv()
            load_half(3).start()
            for i in range(4):
                load_half(i).wait()

            def to_them(b, _, u=u):
                r = pl.ds(pl.multiple_of(ROWS + b * BM, BM), BM)
                theirs[0, pl.ds(pl.multiple_of(b * BM, BM), BM), half_cols(u)] = sum(
                    jnp.dot(h[r, pl.ds(k * D, D)], wt[k, :, half_cols(u)], preferred_element_type=jnp.float32)
                    for k in range(2)
                )
                return 0

            lax.fori_loop(0, ROWS // BM, to_them, 0)
            first_out(theirs, u).start()

    def first_out(theirs, u):
        return pltpu.make_async_remote_copy(
            src_ref=theirs.at[0, :, half_cols(u)], dst_ref=rbuf.at[0, :, half_cols(u)], send_sem=psend.at[0, u],
            recv_sem=precv.at[0, u], device_id=to_x, device_id_type=MESH,
        )

    def both(theirs):
        pl.run_scoped(
            functools.partial(first, theirs=theirs),
            pltpu.VMEM((2 * ROWS, D), jnp.bfloat16),
            pltpu.VMEM((BM, W), jnp.float32),
        )
        pl.run_scoped(
            functools.partial(second, theirs),
            pltpu.VMEM((LAG + 1, ROWS, W), jnp.float32),
            pltpu.VMEM((ROWS, W), jnp.float32),
            pltpu.VMEM((ROWS, W), jnp.bfloat16),
            pltpu.VMEM((2, ROWS, W), jnp.bfloat16),
        )

    def second(theirs, own, back, xb, yb):
        def where(j):
            r, c = lax.rem(j, 4) // 2, 2 * (j // 4) + lax.rem(j, 2)
            return r, c, pl.multiple_of(lax.rem(f + r, 2) * HALF + c * W, W)

        def half_rows(b):
            return pl.ds(pl.multiple_of(b * BM, BM), BM)

        def partial_out(j, b):
            return pltpu.make_async_remote_copy(
                src_ref=theirs.at[lax.rem(j, SLOTS), half_rows(b)], dst_ref=rbuf.at[j, half_rows(b)],
                send_sem=psend.at[j, b], recv_sem=precv.at[j, b], device_id=to_x, device_id_type=MESH,
            )

        def y_out(j, b):
            _, _, at = where(j)
            p = lax.rem(j, 2)
            return pltpu.make_async_copy(
                yb.at[p, half_rows(b)], y.at[half_rows(b), pl.ds(at, W)], loc.at[8 + 2 * p + b]
            )

        def finish(j):
            _, _, at = where(j)
            a = pltpu.make_async_copy(x.at[:, pl.ds(at, W)], xb, loc.at[4])
            a.start()
            halves = [pltpu.make_async_copy(rbuf.at[j, half_rows(b)], back.at[half_rows(b)], loc.at[5 + b]) for b in range(2)]

            @pl.when(j == 0)
            def _():
                for b in range(2):
                    first_out(theirs, b).wait_recv()

            for b in range(2):
                pl.when(j > 0)(lambda b=b: partial_out(j, b).wait_recv())
                halves[b].start()
            pl.when(j >= 2)(lambda: [y_out(j - 2, b).wait() for b in range(2)] and None)
            a.wait()
            for b in range(2):
                halves[b].wait()

                def add(i, _, b=b):
                    r = pl.ds(pl.multiple_of(b * BM + i * 64, 64), 64)
                    total = own[lax.rem(j, LAG + 1), r, :] + back[r, :]
                    yb[lax.rem(j, 2), r, :] = (xb[r, :].astype(jnp.float32) + total).astype(jnp.bfloat16)
                    return 0

                lax.fori_loop(0, BM // 64, add, 0)
                y_out(j, b).start()

        def product(row, b):
            r = pl.ds(pl.multiple_of(row + b * BM, BM), BM)
            return sum(
                jnp.dot(h[r, pl.ds(k * D, D)], wt[k], preferred_element_type=jnp.float32) for k in range(2)
            )

        def chunk(j, _):
            g, q = j // 4, lax.rem(j, 4)
            r, c, _ = where(j)
            pl.when(j == 0)(lambda: slot_a(1, 0 * g, True))
            pl.when((q == 0) & (j > 0))(lambda: slot_a(1, g))
            pl.when(q == 1)(lambda: slot_b(1, g))
            pl.when(q == 2)(lambda: slot_c(1, g))

            def load(sib, s):
                src = g2.at[SIB * sib + 2 * r + s, c]
                return pltpu.make_async_copy(src, wt.at[sib, pl.ds(s * HALF, HALF)], loc.at[2 * sib + s])

            @pl.when((r == 0) & (j > 0))
            def _():
                pltpu.make_async_copy(w2.at[:, cols(c)], wt.at[0, pl.ds(0, HALF)], loc.at[0]).start()

            @pl.when(r == 1)
            def _():
                load(0, 0).start()

            @pl.when(j > 0)
            def _():
                load(0, 1).start()
                for s in range(2):
                    arrived(1, SIB + 2 * r + s, c)
                    load(1, s).start()
                pl.when(j >= SLOTS)(lambda: [partial_out(j - SLOTS, b).wait_send() for b in range(2)] and None)
                for sib in range(2):
                    for s in range(2):
                        load(sib, s).wait()

                def to_them(b, _):
                    theirs[lax.rem(j, SLOTS), half_rows(b), :] = product(ROWS, b)
                    partial_out(j, b).start()
                    return 0

                lax.fori_loop(0, ROWS // BM, to_them, 0)

            def to_us(b, _):
                own[lax.rem(j, LAG + 1), pl.ds(pl.multiple_of(b * BM, BM), BM), :] = product(0, b)
                return 0

            lax.fori_loop(0, ROWS // BM, to_us, 0)
            pl.when(j >= LAG)(lambda: finish(j - LAG))
            return 0

        lax.fori_loop(0, NJ, chunk, 0)

        def drain(j, _):
            finish(j)
            return 0

        lax.fori_loop(NJ - LAG, NJ, drain, 0)
        for j in range(NJ - 2, NJ):
            for b in range(2):
                partial_out(j, b).wait_send()
                y_out(j, b).wait()

    pl.run_scoped(both, pltpu.VMEM((SLOTS, ROWS, W), jnp.float32))

    for u in range(2):
        y_half(u).wait_send()
        y_half_to_sib(u).wait_send()
    for i in range(nx):
        xn_send(i).wait_send()

    def sent(c, _):
        for w in range(2):
            for kind in range(7):
                if w == 1 and kind in (0, 3):
                    pl.when(c > 0)(lambda kind=kind: copy(1, kind, Y, Y, c, to_y).wait_send())
                else:
                    copy(w, kind, Y, Y, c, to_y).wait_send()
        return 0

    lax.fori_loop(0, NC, sent, 0)


def solution(mesh):
    hbm = pl.BlockSpec(memory_space=pltpu.HBM)
    vmem = pl.BlockSpec(memory_space=pltpu.VMEM)

    def body(x, gamma, w1, w2):
        bf16 = functools.partial(jax.ShapeDtypeStruct, dtype=jnp.bfloat16)
        out = pl.pallas_call(
            _kernel,
            out_shape=[
                bf16((ROWS, D)),
                bf16((8, NC, HALF, W)),
                bf16((8, NC, HALF, W)),
                bf16((ROWS, D)),
                bf16((ROWS, D)),
                jax.ShapeDtypeStruct((NJ, ROWS, W), jnp.float32),
            ],
            in_specs=[hbm, vmem, hbm, hbm],
            out_specs=[hbm] * 6,
            scratch_shapes=[
                pltpu.VMEM((2 * ROWS, 4 * HALF), jnp.bfloat16),
                pltpu.VMEM((4, D, W), jnp.bfloat16),
                pltpu.SemaphoreType.DMA((2, 7, NC)),
                pltpu.SemaphoreType.DMA((2, 7, NC)),
                pltpu.SemaphoreType.DMA((ROWS // XR,)),
                pltpu.SemaphoreType.DMA((ROWS // XR,)),
                pltpu.SemaphoreType.DMA((NJ, 2)),
                pltpu.SemaphoreType.DMA((NJ, 2)),
                pltpu.SemaphoreType.DMA((4,)),
                pltpu.SemaphoreType.DMA((4,)),
                pltpu.SemaphoreType.DMA((12,)),
            ],
            compiler_params=pltpu.CompilerParams(
                collective_id=0, has_side_effects=True, vmem_limit_bytes=67_043_328
            ),
            cost_estimate=pl.CostEstimate(flops=275_000_000_000, bytes_accessed=400_000_000, transcendentals=16_777_216),
        )(x, gamma.reshape(1, D), w1, w2)
        return out[0]

    return jax.shard_map(
        body,
        mesh=mesh,
        in_specs=(P(("fsdp", "tp"), None), P(None), P("fsdp", "tp"), P("tp", "fsdp")),
        out_specs=P(("fsdp", "tp"), None),
        check_vma=False,
    )
```

```python
import functools

import jax
import jax.numpy as jnp
from jax import lax
from jax.experimental import pallas as pl
from jax.experimental.pallas import tpu as pltpu
from jax.sharding import PartitionSpec as P

EPS = 1e-6
MESH = pl.DeviceIdType.MESH

ROWS, D, HALF = 1024, 4096, 2048
W = 256
NC = HALF // W
NJ = 2 * NC
BM = 512
XR = 256
LAG = 3
SLOTS = 2
Y, Z, DIAG, SIB = 1, 2, 3, 4


def _kernel(x, gamma, w1, w2, y, o, g1, g2, xnh, xph, rbuf, h, wt, send, recv, xsend, xrecv, psend, precv, dsend, drecv, loc):
    f, t = lax.axis_index("fsdp"), lax.axis_index("tp")
    core, ix, iy = lax.rem(t, 2), lax.rem(t // 2, 2), t // 4
    to_core, to_x, to_y, to_z = (f, t + 1 - 2 * core), (f, t + 2 - 4 * ix), (f, t + 4 - 8 * iy), (1 - f, t)
    shard, got = (w1, w2), (g1, g2)
    mine, other = pl.multiple_of(f * HALF, HALF), pl.multiple_of((1 - f) * HALF, HALF)

    barrier = pltpu.get_barrier_semaphore()
    for d in (to_core, to_x, to_y, to_z):
        pl.semaphore_signal(barrier, inc=1, device_id=d, device_id_type=MESH)
    pl.semaphore_wait(barrier, 4)

    def cols(c):
        return pl.ds(pl.multiple_of(c * W, W), W)

    def copy(w, kind, src, dst_piece, c, device):
        return pltpu.make_async_remote_copy(
            src_ref=shard[w].at[:, cols(c)] if src == 0 else got[w].at[src, c],
            dst_ref=got[w].at[dst_piece, c],
            send_sem=send.at[w, kind, c],
            recv_sem=recv.at[w, dst_piece - 1, c],
            device_id=device,
            device_id_type=MESH,
        )

    def arrived(w, piece, c):
        at = got[w].at[piece, c]
        pltpu.make_async_copy(at, at, recv.at[w, piece - 1, c]).wait()

    def diag_half(k):
        piece, device = ((Z, to_y), (Y, to_z))[k]
        rows = pl.ds(k * HALF // 2, HALF // 2)
        return pltpu.make_async_remote_copy(
            src_ref=g1.at[piece, NC - 1, rows], dst_ref=g1.at[DIAG, NC - 1, rows], send_sem=dsend.at[k],
            recv_sem=drecv.at[k], device_id=device, device_id_type=MESH,
        )

    def own_to_y(w, c):
        copy(w, 0, 0, Y, c, to_y).start()
        copy(w, 2, 0, SIB, c, to_core).start()

    def own_to_z(w, c):
        copy(w, 1, 0, Z, c, to_z).start()

    def to_sib(w, piece, c):
        copy(w, 2 + piece, piece, SIB + piece, c, to_core).start()

    def slot_a(g):
        arrived(0, Y, 2 * g)
        arrived(0, Z, 2 * g + 1)
        copy(0, 6, Y, DIAG, 2 * g, to_z).start()
        if g < 3:
            copy(0, 6, Z, DIAG, 2 * g + 1, to_y).start()
            for k in (2, 3):
                own_to_y(0, 2 * g + k)
                own_to_z(0, 2 * g + 5 - k)
        else:
            diag_half(0).start()
            for c in range(3):
                own_to_y(1, c)
        to_sib(0, Y, 2 * g)
        to_sib(0, Z, 2 * g + 1)

    def slot_b(g):
        arrived(0, Y, 2 * g + 1)
        arrived(0, Z, 2 * g)
        if g == 3:
            diag_half(1).start()
            own_to_z(1, 1)
            own_to_z(1, 0)
        to_sib(0, Y, 2 * g + 1)
        to_sib(0, Z, 2 * g)

    def slot_c(g):
        for c in (2 * g, 2 * g + 1):
            arrived(0, DIAG, c)
            to_sib(0, DIAG, c)

    for c in range(2):
        own_to_y(0, c)
        own_to_z(0, 1 - c)

    def x_in(i):
        return pltpu.make_async_copy(x.at[pl.ds(i * XR, XR)], h.at[pl.ds(i * XR, XR), pl.ds(0, D)], loc.at[i])

    def xn_out(i):
        return pltpu.make_async_copy(h.at[pl.ds(i * XR, XR), pl.ds(0, D)], xnh.at[pl.ds(i * XR, XR)], loc.at[4 + i])

    def xn_send(i):
        rows = pl.ds(i * XR, XR)
        return pltpu.make_async_remote_copy(
            src_ref=xnh.at[rows], dst_ref=xph.at[rows], send_sem=xsend.at[i], recv_sem=xrecv.at[i],
            device_id=to_x, device_id_type=MESH,
        )

    nx = ROWS // XR
    for i in range(nx):
        x_in(i).start()
    for i in range(nx):
        x_in(i).wait()

        def norm(b, _, i=i):
            rows = pl.ds(pl.multiple_of(i * XR + b * 16, 16), 16)
            xf = h[rows, pl.ds(0, D)].astype(jnp.float32)
            mu = jnp.mean(xf, axis=-1, keepdims=True)
            xc = xf - mu
            var = jnp.mean(jnp.square(xc), axis=-1, keepdims=True)
            h[rows, pl.ds(0, D)] = (xc * lax.rsqrt(var + EPS) * gamma[...]).astype(jnp.bfloat16)
            return _

        lax.fori_loop(0, XR // 16, norm, 0)
        xn_out(i).start()
        if i > 0:
            xn_out(i - 1).wait()
            xn_send(i - 1).start()
    xn_out(nx - 1).wait()
    xn_send(nx - 1).start()

    def first(xn, pre, theirs):
        def load_tokens(src, at, row, rows):
            def part(k, column):
                return pltpu.make_async_copy(
                    src.at[pl.ds(at, rows), pl.ds(column, HALF)],
                    xn.at[pl.ds(row, rows), pl.ds(k * HALF, HALF)],
                    loc.at[k],
                )

            for k, column in enumerate((mine, other)):
                part(k, column).start()
            for k, column in enumerate((mine, other)):
                part(k, column).wait()

        def load(unit, slot, q, wait):
            s, by_core, c, core = unit
            cc, cr = c + by_core * q, (1 - by_core) * q + by_core * core

            def start(src, k):
                pltpu.make_async_copy(src, wt.at[slot, pl.ds(k * HALF, HALF)], loc.at[2 * slot + k]).start()

            @pl.when((cr == 0) & (s == 0))
            def _():
                start(w1.at[:, cols(cc)], 0)

            @pl.when((cr == 0) & (s == 1))
            def _():
                start(g1.at[Y, cc], 0)

            @pl.when(cr == 0)
            def _():
                start(g1.at[Z + s, cc], 1)

            @pl.when(cr == 1)
            def _():
                for k in range(2):

                    @pl.when(wait)
                    def _(k=k):
                        arrived(0, SIB + 2 * k + s, cc)

                    start(g1.at[SIB + 2 * k + s, cc], k)

        def store_last(last):
            row, column = last
            at = pl.ds(pl.multiple_of(row, BM), BM), pl.ds(pl.multiple_of(column, W), W)
            h[at] = jax.nn.gelu(pre[...], approximate=True).astype(jnp.bfloat16)

        def run(n, unit, rows, ready, wait, last, ahead=lambda i: 0):
            def load_unit(i):
                ready(i)
                for q in range(2):
                    load(unit(i), 2 * lax.rem(i, 2) + q, q, wait(i))

            def one(i, last):
                pl.when((i == 0) | (i * 0 + ahead(i) < 0))(lambda: load_unit(i))
                hook = lambda m: pl.when((i + 1 < n) & (m == ahead(i + 1)))(lambda: load_unit(i + 1))
                return products(unit(i), 2 * lax.rem(i, 2), rows(i), last, hook)

            return lax.fori_loop(0, n, one, last)

        def products(unit, slot0, rows, last, hook=None):
                s, by_core, c, core = unit
                b0, nb = rows

                def product(m, last):
                    q, b = m // nb, lax.rem(m, nb)
                    slot = slot0 + q

                    @pl.when((b == 0) & (hook is not None))
                    def _():
                        for k in range(2):
                            pltpu.make_async_copy(
                                g1.at[Y, 0], wt.at[slot, pl.ds(k * HALF, HALF)], loc.at[2 * slot + k]
                            ).wait()

                    if hook is not None:
                        hook(m)
                    row = (b0 + b) * BM
                    column = (((1 - by_core) * q + by_core * core) * 2 + s) * HALF + (c + by_core * q) * W
                    store_last(last)
                    r = pl.ds(pl.multiple_of(row, BM), BM)
                    pre[...] = jnp.dot(xn[r, :], wt[slot], preferred_element_type=jnp.float32)
                    return row, column

                return lax.fori_loop(0, 2 * nb, product, last)

        load_tokens(xnh, 0, 0, ROWS)
        zero = lax.rem(core, 1)
        last = (zero, zero + W)
        own_rows, three, early = (0, 2), (0, 3), (2, 1)
        yes, no = (lambda i: i >= 0), (lambda i: i < 0)
        nothing = lambda i: None

        slot_a(0)
        last = run(1, lambda i: (0, 0, 1, 0), lambda i: own_rows, nothing, yes, last)
        slot_b(0)
        last = run(1, lambda i: (0, 0, 0, 0), lambda i: own_rows, nothing, yes, last)
        slot_c(0)
        last = run(2, lambda i: (1, 1, 0, i), lambda i: own_rows, nothing, yes, last, lambda i: 2)
        slot_a(1)
        last = run(1, lambda i: (0, 0, 3, 0), lambda i: own_rows, nothing, yes, last)
        for i in range(nx // 2):
            xn_send(i).wait_recv()
        load_tokens(xph, 0, ROWS, ROWS // 2)
        last = run(4, lambda i: (i // 2, 0, lax.rem(i, 2), 0), lambda i: early, nothing, no, last)
        slot_b(1)
        last = run(1, lambda i: (0, 0, 2, 0), lambda i: three, nothing, yes, last)
        last = run(1, lambda i: (0, 0, 3, 0), lambda i: early, nothing, no, last)
        slot_c(1)
        last = run(2, lambda i: (1, 1, 2, i), lambda i: three, nothing, yes, last, lambda i: 3)
        slot_a(2)
        last = run(1, lambda i: (0, 0, 5, 0), lambda i: three, nothing, yes, last)
        slot_b(2)
        last = run(1, lambda i: (0, 0, 4, 0), lambda i: three, nothing, yes, last)
        for i in range(nx // 2, nx):
            xn_send(i).wait_recv()
        load_tokens(xph, ROWS // 2, ROWS + ROWS // 2, ROWS // 2)

        def unit(i):
            late = i >= 10
            s = jnp.where(late, jnp.where((i == 12) | (i == 13), 0, 1), lax.rem(i // 2, 2))
            s = jnp.where((i == 8) | (i == 9), 0, s)
            by_core = jnp.where(late & (s == 1), 1, 0)
            c = jnp.where(i < 8, 2 * (i // 4) + lax.rem(i, 2), i - 4)
            c = jnp.where(i >= 10, 4, c)
            c = jnp.where(i == 12, 7, c)
            c = jnp.where(i >= 13, 6, c)
            return s, by_core, c, lax.rem(i, 2)

        def rows(i):
            return jnp.where(i >= 10, 0, 3), jnp.where(i >= 10, 4, 1)

        def ready(i):
            pl.when(i == 10)(lambda: slot_c(2))
            pl.when(i == 12)(lambda: slot_a(3))
            pl.when(i == 13)(lambda: slot_b(3))

        def ahead(i):
            return jnp.where(i < 12, 0, jnp.where(i == 12, 4, -1))

        last = run(14, unit, rows, ready, lambda i: i >= 10, last, ahead)

        arrived(0, DIAG, NC - 2)
        to_sib(0, DIAG, NC - 2)
        u = (1, 0, NC - 2, 0)
        load(u, 0, 0, True)
        last = products(u, 0, (0, 4), last, lambda m: pl.when(m == 1)(lambda: load(u, 1, 1, True)))

        for k in range(2):
            diag_half(k).wait_recv()
        to_sib(0, DIAG, NC - 1)
        v = (1, 0, NC - 1, 0)
        load(v, 2, 0, True)
        arrived(1, Y, 0)
        to_sib(1, Y, 0)
        arrived(1, SIB, 0)
        pieces = (w2.at[:, cols(0)], g2.at[Y, 0], g2.at[SIB, 0], g2.at[SIB + Y, 0])

        def load_piece(i):
            return pltpu.make_async_copy(pieces[i], wt.at[i // 2, pl.ds(i % 2 * HALF, HALF)], loc.at[i])

        for i in range(3):
            load_piece(i).start()

        def last_piece():
            arrived(1, SIB + Y, 0)
            load_piece(3).start()

        def hook(m):
            pl.when(m == 1)(lambda: load(v, 3, 1, True))
            pl.when(m == 3)(last_piece)

        last = products(v, 2, (2, 2), last, hook)
        store_last(last)
        for i in range(4):
            load_piece(i).wait()
        partials(theirs, 0)
        last = products(v, 2, own_rows, last)
        store_last(last)

    def half_rows(b):
        return pl.ds(pl.multiple_of(b * BM, BM), BM)

    def partial_out(theirs, j, b):
        return pltpu.make_async_remote_copy(
            src_ref=theirs.at[lax.rem(j, SLOTS), half_rows(b)], dst_ref=rbuf.at[j, half_rows(b)],
            send_sem=psend.at[j, b], recv_sem=precv.at[j, b], device_id=to_x, device_id_type=MESH,
        )

    def second_product(row, b):
        r = pl.ds(pl.multiple_of(row + b * BM, BM), BM)
        return sum(jnp.dot(h[r, pl.ds(k * D, D)], wt[k], preferred_element_type=jnp.float32) for k in range(2))

    def partials(theirs, j):
        def to_them(b, _):
            theirs[lax.rem(j, SLOTS), half_rows(b), :] = second_product(ROWS, b)
            partial_out(theirs, j, b).start()
            return _

        lax.fori_loop(0, ROWS // BM, to_them, 0)

    def both(theirs):
        pl.run_scoped(
            functools.partial(first, theirs=theirs),
            pltpu.VMEM((2 * ROWS, D), jnp.bfloat16),
            pltpu.VMEM((BM, W), jnp.float32),
        )
        pl.run_scoped(
            functools.partial(second, theirs),
            pltpu.VMEM((LAG + 1, ROWS, W), jnp.float32),
            pltpu.VMEM((ROWS, W), jnp.float32),
            pltpu.VMEM((ROWS, W), jnp.bfloat16),
            pltpu.VMEM((2, ROWS, W), jnp.bfloat16),
        )

    def second(theirs, own, back, xb, yb):
        def where(j):
            g, q = (j + 3) // 4 - 1, lax.rem(j + 3, 4)
            r = jnp.where(j >= 14, 1, q // 2)
            c = jnp.where(j >= 14, j - 8, 2 * g + jnp.where(q < 2, q + 1, q - 2))
            r, c = jnp.where(j == 0, 0, r), jnp.where(j == 0, 0, c)
            return r, c, pl.multiple_of(lax.rem(f + r, 2) * HALF + c * W, W)

        def y_out(j, b):
            _, _, at = where(j)
            p = lax.rem(j, 2)
            return pltpu.make_async_copy(
                yb.at[p, half_rows(b)], y.at[half_rows(b), pl.ds(at, W)], loc.at[8 + 2 * p + b]
            )

        def finish(j):
            _, _, at = where(j)
            a = pltpu.make_async_copy(x.at[:, pl.ds(at, W)], xb, loc.at[4])
            a.start()
            halves = [pltpu.make_async_copy(rbuf.at[j, half_rows(b)], back.at[half_rows(b)], loc.at[5 + b]) for b in range(2)]

            for b in range(2):
                partial_out(theirs, j, b).wait_recv()
                halves[b].start()
            pl.when(j >= 2)(lambda: [y_out(j - 2, b).wait() for b in range(2)] and None)
            a.wait()
            for b in range(2):
                halves[b].wait()

                def add(i, _, b=b):
                    r = pl.ds(pl.multiple_of(b * BM + i * 64, 64), 64)
                    total = own[lax.rem(j, LAG + 1), r, :] + back[r, :]
                    yb[lax.rem(j, 2), r, :] = (xb[r, :].astype(jnp.float32) + total).astype(jnp.bfloat16)
                    return _

                lax.fori_loop(0, BM // 64, add, 0)
                y_out(j, b).start()

        def chunk(j, carry):
            g, q = (j + 3) // 4 - 1, lax.rem(j + 3, 4)
            r, c, _ = where(j)

            even = 2 * g
            odd = even + 1

            @pl.when((j > 0) & (q == 0))
            def _():
                arrived(1, Y, odd)
                arrived(1, Z, odd)
                copy(1, 6, Z, DIAG, odd, to_y).start()
                copy(1, 6, Y, DIAG, even, to_z).start()

                @pl.when(g < 3)
                def _():
                    own_to_y(1, odd + 2)
                    own_to_z(1, odd + 2)
                    own_to_z(1, even + 2)

                pl.when(g < 2)(lambda: own_to_y(1, odd + 3))
                to_sib(1, Y, odd)
                to_sib(1, Z, odd)

            @pl.when((j > 0) & (q == 1))
            def _():
                @pl.when(g < 3)
                def _():
                    arrived(1, Y, even + 2)
                    to_sib(1, Y, even + 2)

                arrived(1, Z, even)
                to_sib(1, Z, even)

            @pl.when((j > 0) & (((q == 2) & (g < 3)) | (j == 14)))
            def _():
                for k in range(2):
                    arrived(1, DIAG, even + k)
                    to_sib(1, DIAG, even + k)

            def load(sib, s):
                src = g2.at[SIB * sib + 2 * r + s, c]
                return pltpu.make_async_copy(src, wt.at[sib, pl.ds(s * HALF, HALF)], loc.at[2 * sib + s])

            @pl.when((r == 0) & (j > 0))
            def _():
                pltpu.make_async_copy(w2.at[:, cols(c)], wt.at[0, pl.ds(0, HALF)], loc.at[0]).start()

            @pl.when(r == 1)
            def _():
                load(0, 0).start()

            @pl.when(j > 0)
            def _():
                load(0, 1).start()
                for s in range(2):
                    arrived(1, SIB + 2 * r + s, c)
                    load(1, s).start()
                pl.when(j >= SLOTS)(lambda: [partial_out(theirs, j - SLOTS, b).wait_send() for b in range(2)] and None)
                for sib in range(2):
                    for s in range(2):
                        load(sib, s).wait()

                partials(theirs, j)

            def to_us(b, _):
                own[lax.rem(j, LAG + 1), pl.ds(pl.multiple_of(b * BM, BM), BM), :] = second_product(0, b)
                return _

            lax.fori_loop(0, ROWS // BM, to_us, 0)
            pl.when(j >= LAG)(lambda: finish(j - LAG))
            return carry

        lax.fori_loop(0, NJ, chunk, 0)

        def drain(j, _):
            finish(j)
            return _

        last = NJ - 1
        keep = pltpu.make_async_copy(own.at[last % (LAG + 1)], o, loc.at[0])
        keep.start()
        lax.fori_loop(NJ - LAG, last, drain, 0)
        keep.wait()
        for j in (last, last - 1):
            for b in range(2):
                partial_out(theirs, j, b).wait_send()
                y_out(j - 1, b).wait()
        for b in range(2):
            partial_out(theirs, last, b).wait_recv()

    pl.run_scoped(both, pltpu.VMEM((SLOTS, ROWS, W), jnp.float32))

    for u in range(2):
        diag_half(u).wait_send()
    for i in range(nx):
        xn_send(i).wait_send()

    def sent(c, _):
        for w in range(2):
            for kind in range(7):
                if w == 0 and kind == 6:
                    pl.when(c < NC - 1)(lambda: copy(0, 6, Y, Y, c, to_y).wait_send())
                else:
                    copy(w, kind, Y, Y, c, to_y).wait_send()
        return _

    lax.fori_loop(0, NC, sent, 0)


def _finish(at, x, o, r, y, out, rows, xv, ov, rv, small, came, went):
    n = came.shape[0]
    block = ROWS // n
    columns = pl.ds(pl.multiple_of(at[0], W), W)

    sums = [
        pltpu.make_async_copy(src, dst, small.at[k])
        for k, (src, dst) in enumerate(zip((x.at[:, columns], o, r.at[NJ - 1]), (xv, ov, rv)))
    ]

    def move(i, out_of):
        here, hbm = rows.at[pl.ds(i * block, block)], pl.ds(i * block, block)
        if out_of:
            return pltpu.make_async_copy(here, out.at[hbm], went.at[i])
        return pltpu.make_async_copy(y.at[hbm], here, came.at[i])

    for part in sums:
        part.start()
    for i in range(n):
        move(i, False).start()
    for part in sums:
        part.wait()
    for i in range(n):
        move(i, False).wait()
        b = pl.ds(i * block, block)
        rows[b, columns] = (xv[b, :].astype(jnp.float32) + (ov[b, :] + rv[b, :])).astype(jnp.bfloat16)
        move(i, True).start()
    for i in range(n):
        move(i, True).wait()


def solution(mesh):
    hbm = pl.BlockSpec(memory_space=pltpu.HBM)
    vmem = pl.BlockSpec(memory_space=pltpu.VMEM)

    def body(x, gamma, w1, w2):
        bf16 = functools.partial(jax.ShapeDtypeStruct, dtype=jnp.bfloat16)
        out = pl.pallas_call(
            _kernel,
            out_shape=[
                bf16((ROWS, D)),
                jax.ShapeDtypeStruct((ROWS, W), jnp.float32),
                bf16((8, NC, HALF, W)),
                bf16((8, NC, HALF, W)),
                bf16((ROWS, D)),
                bf16((ROWS, D)),
                jax.ShapeDtypeStruct((NJ, ROWS, W), jnp.float32),
            ],
            in_specs=[hbm, vmem, hbm, hbm],
            out_specs=[hbm] * 7,
            scratch_shapes=[
                pltpu.VMEM((2 * ROWS, 4 * HALF), jnp.bfloat16),
                pltpu.VMEM((4, D, W), jnp.bfloat16),
                pltpu.SemaphoreType.DMA((2, 7, NC)),
                pltpu.SemaphoreType.DMA((2, 7, NC)),
                pltpu.SemaphoreType.DMA((ROWS // XR,)),
                pltpu.SemaphoreType.DMA((ROWS // XR,)),
                pltpu.SemaphoreType.DMA((NJ, 2)),
                pltpu.SemaphoreType.DMA((NJ, 2)),
                pltpu.SemaphoreType.DMA((2,)),
                pltpu.SemaphoreType.DMA((2,)),
                pltpu.SemaphoreType.DMA((12,)),
            ],
            compiler_params=pltpu.CompilerParams(
                collective_id=0, has_side_effects=True, vmem_limit_bytes=67_043_328
            ),
            cost_estimate=pl.CostEstimate(flops=275_000_000_000, bytes_accessed=400_000_000, transcendentals=16_777_216),
        )(x, gamma.reshape(1, D), w1, w2)
        at = lax.rem(lax.axis_index("fsdp") + 1, 2) * HALF + HALF - W
        blocks = 8
        return pl.pallas_call(
            _finish,
            out_shape=bf16((ROWS, D)),
            in_specs=[pl.BlockSpec(memory_space=pltpu.SMEM)] + [hbm] * 4,
            out_specs=hbm,
            scratch_shapes=[
                pltpu.VMEM((ROWS, D), jnp.bfloat16),
                pltpu.VMEM((ROWS, W), jnp.bfloat16),
                pltpu.VMEM((ROWS, W), jnp.float32),
                pltpu.VMEM((ROWS, W), jnp.float32),
                pltpu.SemaphoreType.DMA((3,)),
                pltpu.SemaphoreType.DMA((blocks,)),
                pltpu.SemaphoreType.DMA((blocks,)),
            ],
        )(at.reshape(1), x, out[1], out[-1], out[0])

    return jax.shard_map(
        body,
        mesh=mesh,
        in_specs=(P(("fsdp", "tp"), None), P(None), P("fsdp", "tp"), P("tp", "fsdp")),
        out_specs=P(("fsdp", "tp"), None),
        check_vma=False,
    )
```

```python
import functools

import jax
import jax.numpy as jnp
from jax import lax
from jax.experimental import pallas as pl
from jax.experimental.pallas import tpu as pltpu
from jax.sharding import PartitionSpec as P

EPS = 1e-6
MESH = pl.DeviceIdType.MESH

ROWS, D, HALF = 1024, 4096, 2048
W = 256
NC = HALF // W
NJ = 2 * NC
BM = 512
XR = 256
LAG = 3
SLOTS = 2
LINK, SIBLING = range(2)
Y, Z, DIAG, SIB = 1, 2, 3, 4


def _kernel(x, gamma, w1, w2, y, o, g1, g2, xnh, xph, rbuf, h, wt, send, recv, xsend, xrecv, psend, precv, dsend, drecv, loc):
    f, t = lax.axis_index("fsdp"), lax.axis_index("tp")
    core, ix, iy = lax.rem(t, 2), lax.rem(t // 2, 2), t // 4
    to_core, to_x, to_y, to_z = (f, t + 1 - 2 * core), (f, t + 2 - 4 * ix), (f, t + 4 - 8 * iy), (1 - f, t)
    shard, got = (w1, w2), (g1, g2)
    mine, other = pl.multiple_of(f * HALF, HALF), pl.multiple_of((1 - f) * HALF, HALF)

    barrier = pltpu.get_barrier_semaphore()
    for d in (to_core, to_x, to_y, to_z):
        pl.semaphore_signal(barrier, inc=1, device_id=d, device_id_type=MESH)
    pl.semaphore_wait(barrier, 4)

    def cols(c):
        return pl.ds(pl.multiple_of(c * W, W), W)

    def copy(w, kind, src, dst_piece, c, device):
        return pltpu.make_async_remote_copy(
            src_ref=shard[w].at[:, cols(c)] if src == 0 else got[w].at[src, c],
            dst_ref=got[w].at[dst_piece, c],
            send_sem=send.at[w, kind, c],
            recv_sem=recv.at[w, dst_piece - 1, c],
            device_id=device,
            device_id_type=MESH,
        )

    def arrived(w, piece, c):
        at = got[w].at[piece, c]
        pltpu.make_async_copy(at, at, recv.at[w, piece - 1, c]).wait()

    def diag_half(k, sib):
        piece, device = ((Z, to_y), (Y, to_z))[k]
        if sib:
            piece, device = DIAG, to_core
        rows = pl.ds(k * HALF // 2, HALF // 2)
        i = 2 * sib + k
        return pltpu.make_async_remote_copy(
            src_ref=g1.at[piece, NC - 1, rows], dst_ref=g1.at[SIB * sib + DIAG, NC - 1, rows], send_sem=dsend.at[i],
            recv_sem=drecv.at[i], device_id=device, device_id_type=MESH,
        )

    def pass_half(k):
        diag_half(k, LINK).wait_recv()
        diag_half(k, SIBLING).start()

    def own_to_y(w, c):
        copy(w, 0, 0, Y, c, to_y).start()
        copy(w, 2, 0, SIB, c, to_core).start()

    def own_to_z(w, c):
        copy(w, 1, 0, Z, c, to_z).start()

    def to_sib(w, piece, c):
        copy(w, 2 + piece, piece, SIB + piece, c, to_core).start()

    def slot_a(g):
        arrived(0, Y, 2 * g)
        arrived(0, Z, 2 * g + 1)
        copy(0, 6, Y, DIAG, 2 * g, to_z).start()
        if g < 3:
            copy(0, 6, Z, DIAG, 2 * g + 1, to_y).start()
            for k in (2, 3):
                own_to_y(0, 2 * g + k)
                own_to_z(0, 2 * g + 5 - k)
        else:
            diag_half(0, LINK).start()
            for c in range(3):
                own_to_y(1, c)
        to_sib(0, Y, 2 * g)
        to_sib(0, Z, 2 * g + 1)

    def slot_b(g):
        arrived(0, Y, 2 * g + 1)
        arrived(0, Z, 2 * g)
        if g == 3:
            diag_half(1, LINK).start()
            own_to_z(1, 1)
            own_to_z(1, 0)
        to_sib(0, Y, 2 * g + 1)
        to_sib(0, Z, 2 * g)

    def slot_c(g):
        for c in (2 * g, 2 * g + 1):
            arrived(0, DIAG, c)
            to_sib(0, DIAG, c)

    for c in range(2):
        own_to_y(0, c)
        own_to_z(0, 1 - c)

    def x_in(i):
        return pltpu.make_async_copy(x.at[pl.ds(i * XR, XR)], h.at[pl.ds(i * XR, XR), pl.ds(0, D)], loc.at[i])

    def xn_out(i):
        return pltpu.make_async_copy(h.at[pl.ds(i * XR, XR), pl.ds(0, D)], xnh.at[pl.ds(i * XR, XR)], loc.at[4 + i])

    def xn_send(i):
        rows = pl.ds(i * XR, XR)
        return pltpu.make_async_remote_copy(
            src_ref=xnh.at[rows], dst_ref=xph.at[rows], send_sem=xsend.at[i], recv_sem=xrecv.at[i],
            device_id=to_x, device_id_type=MESH,
        )

    nx = ROWS // XR
    for i in range(nx):
        x_in(i).start()
    for i in range(nx):
        x_in(i).wait()

        def norm(b, _, i=i):
            rows = pl.ds(pl.multiple_of(i * XR + b * 16, 16), 16)
            xf = h[rows, pl.ds(0, D)].astype(jnp.float32)
            mu = jnp.mean(xf, axis=-1, keepdims=True)
            xc = xf - mu
            var = jnp.mean(jnp.square(xc), axis=-1, keepdims=True)
            h[rows, pl.ds(0, D)] = (xc * lax.rsqrt(var + EPS) * gamma[...]).astype(jnp.bfloat16)
            return _

        lax.fori_loop(0, XR // 16, norm, 0)
        xn_out(i).start()
        if i > 0:
            xn_out(i - 1).wait()
            xn_send(i - 1).start()
    xn_out(nx - 1).wait()
    xn_send(nx - 1).start()

    def first(xn, pre, theirs):
        def load_tokens(src, at, row, rows):
            def part(k, column):
                return pltpu.make_async_copy(
                    src.at[pl.ds(at, rows), pl.ds(column, HALF)],
                    xn.at[pl.ds(row, rows), pl.ds(k * HALF, HALF)],
                    loc.at[k],
                )

            for k, column in enumerate((mine, other)):
                part(k, column).start()
            for k, column in enumerate((mine, other)):
                part(k, column).wait()

        def load(unit, slot, q, wait):
            s, by_core, c, core = unit
            cc, cr = c + by_core * q, (1 - by_core) * q + by_core * core

            def start(src, k):
                pltpu.make_async_copy(src, wt.at[slot, pl.ds(k * HALF, HALF)], loc.at[2 * slot + k]).start()

            @pl.when((cr == 0) & (s == 0))
            def _():
                start(w1.at[:, cols(cc)], 0)

            @pl.when((cr == 0) & (s == 1))
            def _():
                start(g1.at[Y, cc], 0)

            @pl.when(cr == 0)
            def _():
                start(g1.at[Z + s, cc], 1)

            @pl.when(cr == 1)
            def _():
                for k in range(2):

                    @pl.when(wait)
                    def _(k=k):
                        arrived(0, SIB + 2 * k + s, cc)

                    start(g1.at[SIB + 2 * k + s, cc], k)

        def store_last(last):
            row, column = last
            at = pl.ds(pl.multiple_of(row, BM), BM), pl.ds(pl.multiple_of(column, W), W)
            h[at] = jax.nn.gelu(pre[...], approximate=True).astype(jnp.bfloat16)

        def run(n, unit, rows, ready, wait, last, ahead=lambda i: 0):
            def load_unit(i):
                ready(i)
                for q in range(2):
                    load(unit(i), 2 * lax.rem(i, 2) + q, q, wait(i))

            def one(i, last):
                pl.when((i == 0) | (i * 0 + ahead(i) < 0))(lambda: load_unit(i))
                hook = lambda m: pl.when((i + 1 < n) & (m == ahead(i + 1)))(lambda: load_unit(i + 1))
                return products(unit(i), 2 * lax.rem(i, 2), rows(i), last, hook)

            return lax.fori_loop(0, n, one, last)

        def products(unit, slot0, rows, last, hook=None):
                s, by_core, c, core = unit
                b0, nb = rows

                def product(m, last):
                    q, b = m // nb, lax.rem(m, nb)
                    slot = slot0 + q

                    @pl.when((b == 0) & (hook is not None))
                    def _():
                        for k in range(2):
                            pltpu.make_async_copy(
                                g1.at[Y, 0], wt.at[slot, pl.ds(k * HALF, HALF)], loc.at[2 * slot + k]
                            ).wait()

                    if hook is not None:
                        hook(m)
                    row = (b0 + b) * BM
                    column = (((1 - by_core) * q + by_core * core) * 2 + s) * HALF + (c + by_core * q) * W
                    store_last(last)
                    r = pl.ds(pl.multiple_of(row, BM), BM)
                    pre[...] = jnp.dot(xn[r, :], wt[slot], preferred_element_type=jnp.float32)
                    return row, column

                return lax.fori_loop(0, 2 * nb, product, last)

        load_tokens(xnh, 0, 0, ROWS)
        zero = core - core
        last = (zero, zero + W)
        own_rows, three, early = (0, 2), (0, 3), (2, 1)
        yes, no = (lambda i: i >= 0), (lambda i: i < 0)
        nothing = lambda i: None

        slot_a(0)
        last = run(1, lambda i: (0, 0, 1, 0), lambda i: own_rows, nothing, yes, last)
        slot_b(0)
        last = run(1, lambda i: (0, 0, 0, 0), lambda i: own_rows, nothing, yes, last)
        slot_c(0)
        last = run(2, lambda i: (1, 1, 0, i), lambda i: own_rows, nothing, yes, last, lambda i: 2)
        slot_a(1)
        last = run(1, lambda i: (0, 0, 3, 0), lambda i: own_rows, nothing, yes, last)
        for i in range(nx // 2):
            xn_send(i).wait_recv()
        load_tokens(xph, 0, ROWS, ROWS // 2)
        last = run(4, lambda i: (i // 2, 0, lax.rem(i, 2), 0), lambda i: early, nothing, no, last)
        slot_b(1)
        last = run(1, lambda i: (0, 0, 2, 0), lambda i: three, nothing, yes, last)
        last = run(1, lambda i: (0, 0, 3, 0), lambda i: early, nothing, no, last)
        slot_c(1)
        last = run(2, lambda i: (1, 1, 2, i), lambda i: three, nothing, yes, last, lambda i: 3)
        slot_a(2)
        last = run(1, lambda i: (0, 0, 5, 0), lambda i: three, nothing, yes, last)
        slot_b(2)
        last = run(1, lambda i: (0, 0, 4, 0), lambda i: three, nothing, yes, last)
        for i in range(nx // 2, nx):
            xn_send(i).wait_recv()
        load_tokens(xph, ROWS // 2, ROWS + ROWS // 2, ROWS // 2)

        def unit(i):
            late = i >= 10
            s = jnp.where(late, jnp.where((i == 12) | (i == 13), 0, 1), lax.rem(i // 2, 2))
            s = jnp.where((i == 8) | (i == 9), 0, s)
            by_core = jnp.where(late & (s == 1), 1, 0)
            c = jnp.where(i < 8, 2 * (i // 4) + lax.rem(i, 2), i - 4)
            c = jnp.where(i >= 10, 4, c)
            c = jnp.where(i == 12, 7, c)
            c = jnp.where(i >= 13, 6, c)
            return s, by_core, c, lax.rem(i, 2)

        def rows(i):
            return jnp.where(i >= 10, 0, 3), jnp.where(i >= 10, 4, 1)

        def ready(i):
            pl.when(i == 10)(lambda: slot_c(2))
            pl.when(i == 12)(lambda: slot_a(3))
            pl.when(i == 13)(lambda: slot_b(3))

        def ahead(i):
            return jnp.where(i < 12, 0, jnp.where(i == 12, 4, -1))

        last = run(14, unit, rows, ready, lambda i: i >= 10, last, ahead)

        arrived(0, DIAG, NC - 2)
        to_sib(0, DIAG, NC - 2)
        pass_half(0)
        u = (1, 0, NC - 2, 0)
        load(u, 0, 0, True)
        last = products(u, 0, (0, 4), last, lambda m: pl.when(m == 1)(lambda: load(u, 1, 1, True)))

        pass_half(1)
        v = (1, 0, NC - 1, 0)
        load(v, 2, 0, True)
        arrived(1, Y, 0)
        to_sib(1, Y, 0)
        arrived(1, SIB, 0)
        pieces = (w2.at[:, cols(0)], g2.at[Y, 0], g2.at[SIB, 0], g2.at[SIB + Y, 0])

        def load_piece(i):
            return pltpu.make_async_copy(pieces[i], wt.at[i // 2, pl.ds(i % 2 * HALF, HALF)], loc.at[i])

        for i in range(3):
            load_piece(i).start()

        def last_piece():
            arrived(1, SIB + Y, 0)
            load_piece(3).start()

        def other_tile():
            arrived(0, SIB + Y, NC - 1)
            for k in range(2):
                diag_half(k, SIBLING).wait_recv()
            load(v, 3, 1, core < 0)

        def hook(m):
            pl.when(m == 1)(other_tile)
            pl.when(m == 3)(last_piece)

        last = products(v, 2, (2, 2), last, hook)
        store_last(last)
        for i in range(4):
            load_piece(i).wait()
        partials(theirs, 0)
        last = products(v, 2, own_rows, last)
        store_last(last)

    def half_rows(b):
        return pl.ds(pl.multiple_of(b * BM, BM), BM)

    def partial_out(theirs, j, b):
        return pltpu.make_async_remote_copy(
            src_ref=theirs.at[lax.rem(j, SLOTS), half_rows(b)], dst_ref=rbuf.at[j, half_rows(b)],
            send_sem=psend.at[j, b], recv_sem=precv.at[j, b], device_id=to_x, device_id_type=MESH,
        )

    def second_product(row, b):
        r = pl.ds(pl.multiple_of(row + b * BM, BM), BM)
        return sum(jnp.dot(h[r, pl.ds(k * D, D)], wt[k], preferred_element_type=jnp.float32) for k in range(2))

    def partials(theirs, j):
        def to_them(b, _):
            theirs[lax.rem(j, SLOTS), half_rows(b), :] = second_product(ROWS, b)
            partial_out(theirs, j, b).start()
            return _

        lax.fori_loop(0, ROWS // BM, to_them, 0)

    def settle():
        for u in range(2):
            diag_half(u, LINK).wait_send()
            diag_half(u, SIBLING).wait_send()
        for i in range(nx):
            xn_send(i).wait_send()

        def sent(c, _):
            for w in range(2):
                for kind in range(7):
                    if w == 0 and kind > 4:
                        pl.when(c < NC - 1)(lambda kind=kind: copy(0, kind, Y, Y, c, to_y).wait_send())
                    else:
                        copy(w, kind, Y, Y, c, to_y).wait_send()
            return _

        lax.fori_loop(0, NC, sent, 0)

    def both(theirs):
        pl.run_scoped(
            functools.partial(first, theirs=theirs),
            pltpu.VMEM((2 * ROWS, D), jnp.bfloat16),
            pltpu.VMEM((BM, W), jnp.float32),
        )
        pl.run_scoped(
            functools.partial(second, theirs),
            pltpu.VMEM((LAG + 1, ROWS, W), jnp.float32),
            pltpu.VMEM((ROWS, W), jnp.float32),
            pltpu.VMEM((ROWS, W), jnp.bfloat16),
            pltpu.VMEM((2, ROWS, W), jnp.bfloat16),
        )

    def second(theirs, own, back, xb, yb):
        def where(j):
            g, q = (j + 3) // 4 - 1, lax.rem(j + 3, 4)
            r = jnp.where(j >= 14, 1, q // 2)
            c = jnp.where(j >= 14, j - 8, 2 * g + jnp.where(q < 2, q + 1, q - 2))
            r, c = jnp.where(j == 0, 0, r), jnp.where(j == 0, 0, c)
            return r, c, pl.multiple_of(lax.rem(f + r, 2) * HALF + c * W, W)

        def y_out(j, b):
            _, _, at = where(j)
            p = lax.rem(j, 2)
            return pltpu.make_async_copy(
                yb.at[p, half_rows(b)], y.at[half_rows(b), pl.ds(at, W)], loc.at[8 + 2 * p + b]
            )

        def finish(j):
            _, _, at = where(j)
            a = pltpu.make_async_copy(x.at[:, pl.ds(at, W)], xb, loc.at[4])
            a.start()
            halves = [pltpu.make_async_copy(rbuf.at[j, half_rows(b)], back.at[half_rows(b)], loc.at[5 + b]) for b in range(2)]

            for b in range(2):
                partial_out(theirs, j, b).wait_recv()
                halves[b].start()
            pl.when(j >= 2)(lambda: [y_out(j - 2, b).wait() for b in range(2)] and None)
            a.wait()
            for b in range(2):
                halves[b].wait()

                def add(i, _, b=b):
                    r = pl.ds(pl.multiple_of(b * BM + i * 64, 64), 64)
                    total = own[lax.rem(j, LAG + 1), r, :] + back[r, :]
                    yb[lax.rem(j, 2), r, :] = (xb[r, :].astype(jnp.float32) + total).astype(jnp.bfloat16)
                    return _

                lax.fori_loop(0, BM // 64, add, 0)
                y_out(j, b).start()

        def chunk(j, carry):
            g, q = (j + 3) // 4 - 1, lax.rem(j + 3, 4)
            r, c, _ = where(j)

            even = 2 * g
            odd = even + 1

            @pl.when((j > 0) & (q == 0))
            def _():
                arrived(1, Y, odd)
                to_sib(1, Y, odd)
                arrived(1, Z, odd)
                copy(1, 6, Z, DIAG, odd, to_y).start()
                copy(1, 6, Y, DIAG, even, to_z).start()

                @pl.when(g < 3)
                def _():
                    own_to_y(1, odd + 2)
                    own_to_z(1, odd + 2)
                    own_to_z(1, even + 2)

                pl.when(g < 2)(lambda: own_to_y(1, odd + 3))
                to_sib(1, Z, odd)

            @pl.when((j > 0) & (q == 1))
            def _():
                @pl.when(g < 3)
                def _():
                    arrived(1, Y, even + 2)
                    to_sib(1, Y, even + 2)

                arrived(1, Z, even)
                to_sib(1, Z, even)

            @pl.when((j > 0) & (((q == 2) & (g < 3)) | (j == 14)))
            def _():
                for k in range(2):
                    arrived(1, DIAG, even + k)
                    to_sib(1, DIAG, even + k)

            def load(sib, s):
                src = g2.at[SIB * sib + 2 * r + s, c]
                return pltpu.make_async_copy(src, wt.at[sib, pl.ds(s * HALF, HALF)], loc.at[2 * sib + s])

            @pl.when((r == 0) & (j > 0))
            def _():
                pltpu.make_async_copy(w2.at[:, cols(c)], wt.at[0, pl.ds(0, HALF)], loc.at[0]).start()

            @pl.when(r == 1)
            def _():
                load(0, 0).start()

            @pl.when(j > 0)
            def _():
                load(0, 1).start()
                for s in range(2):
                    arrived(1, SIB + 2 * r + s, c)
                    load(1, s).start()
                pl.when(j >= SLOTS)(lambda: [partial_out(theirs, j - SLOTS, b).wait_send() for b in range(2)] and None)
                for sib in range(2):
                    for s in range(2):
                        load(sib, s).wait()

                partials(theirs, j)

            def to_us(b, _):
                own[lax.rem(j, LAG + 1), pl.ds(pl.multiple_of(b * BM, BM), BM), :] = second_product(0, b)
                return _

            lax.fori_loop(0, ROWS // BM, to_us, 0)
            pl.when(j >= LAG)(lambda: finish(j - LAG))
            return carry

        lax.fori_loop(0, NJ, chunk, 0)

        def drain(j, _):
            finish(j)
            return _

        last = NJ - 1
        keep = pltpu.make_async_copy(own.at[last % (LAG + 1)], o, loc.at[0])
        keep.start()
        lax.fori_loop(NJ - LAG, last, drain, 0)
        keep.wait()
        settle()
        for j in (last, last - 1):
            for b in range(2):
                partial_out(theirs, j, b).wait_send()
                y_out(j - 1, b).wait()
        for b in range(2):
            partial_out(theirs, last, b).wait_recv()

    pl.run_scoped(both, pltpu.VMEM((SLOTS, ROWS, W), jnp.float32))


def _finish(at, x, o, r, y, out, rows, xv, ov, rv, small, came, went):
    n = came.shape[0]
    block = ROWS // n
    columns = pl.ds(pl.multiple_of(at[0], W), W)

    sums = [
        pltpu.make_async_copy(src, dst, small.at[k])
        for k, (src, dst) in enumerate(zip((x.at[:, columns], o, r.at[NJ - 1]), (xv, ov, rv)))
    ]

    def move(i, out_of):
        here, hbm = rows.at[pl.ds(i * block, block)], pl.ds(i * block, block)
        if out_of:
            return pltpu.make_async_copy(here, out.at[hbm], went.at[i])
        return pltpu.make_async_copy(y.at[hbm], here, came.at[i])

    for part in sums:
        part.start()
    for i in range(n):
        move(i, False).start()
    for part in sums:
        part.wait()
    for i in range(n):
        move(i, False).wait()
        b = pl.ds(i * block, block)
        rows[b, columns] = (xv[b, :].astype(jnp.float32) + (ov[b, :] + rv[b, :])).astype(jnp.bfloat16)
        move(i, True).start()
    for i in range(n):
        move(i, True).wait()


def solution(mesh):
    hbm = pl.BlockSpec(memory_space=pltpu.HBM)
    vmem = pl.BlockSpec(memory_space=pltpu.VMEM)

    def body(x, gamma, w1, w2):
        bf16 = functools.partial(jax.ShapeDtypeStruct, dtype=jnp.bfloat16)
        out = pl.pallas_call(
            _kernel,
            out_shape=[
                bf16((ROWS, D)),
                jax.ShapeDtypeStruct((ROWS, W), jnp.float32),
                bf16((8, NC, HALF, W)),
                bf16((8, NC, HALF, W)),
                bf16((ROWS, D)),
                bf16((ROWS, D)),
                jax.ShapeDtypeStruct((NJ, ROWS, W), jnp.float32),
            ],
            in_specs=[hbm, vmem, hbm, hbm],
            out_specs=[hbm] * 7,
            scratch_shapes=[
                pltpu.VMEM((2 * ROWS, 4 * HALF), jnp.bfloat16),
                pltpu.VMEM((4, D, W), jnp.bfloat16),
                pltpu.SemaphoreType.DMA((2, 7, NC)),
                pltpu.SemaphoreType.DMA((2, 7, NC)),
                pltpu.SemaphoreType.DMA((ROWS // XR,)),
                pltpu.SemaphoreType.DMA((ROWS // XR,)),
                pltpu.SemaphoreType.DMA((NJ, 2)),
                pltpu.SemaphoreType.DMA((NJ, 2)),
                pltpu.SemaphoreType.DMA((4,)),
                pltpu.SemaphoreType.DMA((4,)),
                pltpu.SemaphoreType.DMA((12,)),
            ],
            compiler_params=pltpu.CompilerParams(
                collective_id=0, has_side_effects=True, vmem_limit_bytes=67_043_328
            ),
            cost_estimate=pl.CostEstimate(flops=275_000_000_000, bytes_accessed=400_000_000, transcendentals=16_777_216),
        )(x, gamma.reshape(1, D), w1, w2)
        at = lax.rem(lax.axis_index("fsdp") + 1, 2) * HALF + HALF - W
        blocks = 16
        return pl.pallas_call(
            _finish,
            out_shape=bf16((ROWS, D)),
            in_specs=[pl.BlockSpec(memory_space=pltpu.SMEM)] + [hbm] * 4,
            out_specs=hbm,
            scratch_shapes=[
                pltpu.VMEM((ROWS, D), jnp.bfloat16),
                pltpu.VMEM((ROWS, W), jnp.bfloat16),
                pltpu.VMEM((ROWS, W), jnp.float32),
                pltpu.VMEM((ROWS, W), jnp.float32),
                pltpu.SemaphoreType.DMA((3,)),
                pltpu.SemaphoreType.DMA((blocks,)),
                pltpu.SemaphoreType.DMA((blocks,)),
            ],
        )(at.reshape(1), x, out[1], out[-1], out[0])

    return jax.shard_map(
        body,
        mesh=mesh,
        in_specs=(P(("fsdp", "tp"), None), P(None), P("fsdp", "tp"), P("tp", "fsdp")),
        out_specs=P(("fsdp", "tp"), None),
        check_vma=False,
    )
```
